32 devices in a mesh: gr: 8 (over y, x, core), gc: 4 (over z).
Axes of the slice: x: 2, y: 2, z: 4, core: 2. Of those that a mesh axis runs over, the one named last changes fastest.
Arguments:
- returns: bfloat16 [4096, 8192], P(('gr', 'gc')), may hold values from -6 to 6
- start_seed: int32 [8192, 64], replicated, may hold values from -1000 to 999
Outputs:
- loadings: float32 [8192, 64], P('gr')
- strengths: float32 [3, 64], replicated
The draws below stay inside these ranges and needn't reach their ends.
All inputs are finite; a program needn't handle non-finite values.
Results may differ from the reference program's by a relative error of at most 0.0003.
Values may be sent and summed in bfloat16 or wider, within the bound.
No kernel may reach another device: no remote copies, remote signals or barrier semaphores. Data moves between devices by JAX's collectives and lax.ppermute only.
A program may use at most 128 MiB of HBM per device.

```python
import math
import jax
import jax.numpy as jnp
from jax import lax

ASSETS = 8192
FACTORS = 64
ITERS = 3
DAYS = 4096


def with_ends(entries, own_key, low, high):
    index_at = [jax.random.randint(jax.random.fold_in(own_key, axis), (), 0, length) for axis, length in enumerate(entries.shape)]
    longest = entries.shape.index(max(entries.shape))
    next_to = index_at[:longest] + [(index_at[longest] + 1) % entries.shape[longest]] + index_at[longest + 1:]
    return entries.at[tuple(index_at)].set(low).at[tuple(next_to)].set(high)


def levels(key, shape, cuts, least, top_value):
    def one(dim, parts):
        steps = jax.random.uniform(jax.random.fold_in(jax.random.fold_in(key, 6), dim), (parts,), jnp.float32, least / len(cuts), top_value / len(cuts))
        return jnp.repeat(jnp.exp(steps), shape[dim] // parts).reshape((-1,) + (1,) * (len(shape) - dim - 1))

    gain = one(*cuts[0])
    for cut in cuts[1:]:
        gain = gain * one(*cut)
    return gain


def normal_values(rng, dims, deviation, bound, cuts=(), dtype=jnp.bfloat16):
    entries = deviation * jax.random.normal(rng, dims, jnp.float32)
    if cuts:
        entries = entries * levels(rng, dims, cuts, -0.22, 0.18)
    return jnp.clip(entries, -bound, bound).astype(dtype)


def setup_inputs(seed: int = 0) -> dict:
    key_of = jax.random.split(jax.random.key(seed), 3)
    returns = normal_values(key_of[0], (DAYS, ASSETS), 1.0, 6.0, ((0, 32),))
    start_seed = with_ends(jax.random.randint(key_of[1], (ASSETS, FACTORS), -1000, 1000), jax.random.fold_in(key_of[1], 1), -1000, 999).astype(jnp.int32)
    return dict(returns=returns, start_seed=start_seed)


def orthonormal(applied):
    inner_gram = jnp.dot(applied.T, applied, precision=lax.Precision.HIGHEST)
    factor = jnp.linalg.cholesky(inner_gram)
    solved = lax.linalg.triangular_solve(factor, applied, left_side=False, lower=True, transpose_a=True)
    return (solved, jnp.diagonal(factor))

def reference(returns, start_seed):
    covariance = jnp.dot(returns.T.astype(jnp.float32), returns.astype(jnp.float32), preferred_element_type=jnp.float32) / DAYS
    vectors = start_seed.astype(jnp.float32) / 1000.0
    diagonals = []
    for sweep in range(ITERS):
        applied = jnp.dot(covariance, vectors, precision=lax.Precision.HIGHEST)
        vectors, diag_part = orthonormal(applied)
        diagonals.append(diag_part)
    return (vectors * math.sqrt(ASSETS), jnp.stack(diagonals, axis=0))
```

```python
import functools
import math

import jax
import jax.numpy as jnp
from jax import lax
from jax.experimental import pallas as pl
from jax.experimental.pallas import tpu as pltpu
from jax.sharding import PartitionSpec as P

ITERS = 3
LANES = 128
HIGH = lax.Precision.HIGHEST
F32 = jnp.float32
BF16 = jnp.bfloat16


def vmem(count):
    return [pl.BlockSpec(memory_space=pltpu.VMEM)] * count


def smem():
    return [pl.BlockSpec(memory_space=pltpu.SMEM)]


def call(body, outs, scalars, arrays, flops, scratch=()):
    in_specs = smem() * len(scalars) + vmem(len(arrays))
    moved = sum(math.prod(o[0]) * 4 for o in outs)
    return pl.pallas_call(
        body,
        out_shape=[jax.ShapeDtypeStruct(shape, dtype) for shape, dtype in outs],
        in_specs=in_specs,
        out_specs=vmem(len(outs)),
        scratch_shapes=list(scratch),
        cost_estimate=pl.CostEstimate(flops=flops, bytes_accessed=moved, transcendentals=0),
        compiler_params=pltpu.CompilerParams(vmem_limit_bytes=40 * 1024 * 1024),
    )(*scalars, *arrays)


def thirds(x):
    top = x.astype(BF16)
    rest = x - top.astype(F32)
    mid = rest.astype(BF16)
    low = (rest - mid.astype(F32)).astype(BF16)
    return top, mid, low


def fold(tall, rows):
    return tall[2 * rows :] + tall[rows : 2 * rows] + tall[:rows]


def widths(x_ref, blocks, span):
    return [x_ref[:, pl.ds(b * span, span)] for b in range(blocks)]


def first_body(returns_ref, seed_ref, out_ref):
    blocks, days, wide = out_ref.shape
    span = returns_ref.shape[1] // blocks
    factors = seed_ref.shape[1]
    seed = seed_ref[...]
    coarse = (seed >> 3) << 3
    fine = seed - coarse
    both = jnp.concatenate([coarse.astype(F32), fine.astype(F32)], axis=1).astype(BF16)
    tall = jnp.dot(returns_ref[...], both, preferred_element_type=F32)
    projected = (tall[:, :factors] + tall[:, factors:]) / 1000.0
    top, mid, low = thirds(projected)
    pad = jnp.zeros((days, wide - span - 3 * factors), BF16)
    tail = jnp.concatenate([top, mid, low, pad], axis=1)
    for b in range(blocks):
        out_ref[b, :, :span] = returns_ref[:, b * span : (b + 1) * span]
        out_ref[b, :, span:] = tail


def halves(par_ref, full_ref, keep_ref, send_ref):
    rows = keep_ref.shape[0]
    at = pl.multiple_of(par_ref[0] * rows, 8)
    other = pl.multiple_of((1 - par_ref[0]) * rows, 8)
    keep_ref[...] = full_ref[pl.ds(at, rows), :]
    send_ref[...] = full_ref[pl.ds(other, rows), :]


def joined(par_ref, mine_ref, theirs_ref, full_ref):
    rows = mine_ref.shape[0]
    at = pl.multiple_of(par_ref[0] * rows, 8)
    other = pl.multiple_of((1 - par_ref[0]) * rows, 8)
    full_ref[pl.ds(at, rows), :] = mine_ref[...]
    full_ref[pl.ds(other, rows), :] = theirs_ref[...]


def apply_first_body(span, par_ref, block_ref, keep_ref, send_ref, full_ref):
    factors = full_ref.shape[0]
    tall = lax.dot_general(
        block_ref[:, span : span + 3 * factors],
        block_ref[:, :span],
        (((0,), (0,)), ((), ())),
        preferred_element_type=F32,
    )
    full_ref[...] = fold(tall, factors)
    halves(par_ref, full_ref, keep_ref, send_ref)


def apply_body(span, core_ref, par_ref, mine_ref, theirs_ref, block_ref, keep_ref, send_ref, proj_ref, full_ref):
    joined(core_ref, mine_ref, theirs_ref, proj_ref)
    factors = full_ref.shape[0]
    days = block_ref.shape[0]
    parts = jnp.concatenate(thirds(proj_ref[:, :days]), axis=0)
    tall = jnp.dot(parts, block_ref[:, :span], preferred_element_type=F32)
    full_ref[...] = fold(tall, factors)
    halves(par_ref, full_ref, keep_ref, send_ref)


def gram_of(applied):
    return lax.dot_general(applied, applied, (((1,), (1,)), ((), ())), precision=HIGH, preferred_element_type=F32)


def project_body(days_all, scaled, span, par_ref, core_ref, mine_ref, theirs_ref, block_ref, *rest):
    if scaled:
        inv_ref, keep_ref, send_ref, full_ref, out_ref = rest
    else:
        keep_ref, send_ref, full_ref, out_ref = rest
    joined(par_ref, mine_ref, theirs_ref, full_ref)
    factors = full_ref.shape[0]
    applied = full_ref[...] / days_all
    if scaled:
        applied = jnp.dot(inv_ref[...], applied, precision=HIGH, preferred_element_type=F32)
    days = block_ref.shape[0]
    parts = jnp.concatenate(thirds(applied), axis=0)
    tall = lax.dot_general(
        parts, block_ref[:, :span], (((1,), (1,)), ((), ())), preferred_element_type=F32
    )
    out_ref[:, :days] = fold(tall, factors)
    out_ref[:, days:] = jnp.concatenate(
        [gram_of(applied), jnp.zeros((factors, out_ref.shape[1] - days - factors), F32)], axis=1
    )
    halves(core_ref, out_ref, keep_ref, send_ref)


def eliminate(gram):
    size = gram.shape[0]
    rows = lax.broadcasted_iota(jnp.int32, (size, 2 * size), 0)
    lanes = lax.broadcasted_iota(jnp.int32, (size, 2 * size), 1)
    work = jnp.concatenate([gram, jnp.zeros_like(gram)], axis=1)
    work = jnp.where(lanes == rows + size, 1.0, work)
    for k in range(size - 1):
        pivot_row = work[k : k + 1, :]
        scaled_row = pivot_row / work[k : k + 1, k : k + 1]
        column = jnp.where(rows[:, :1] > k, work[:, k : k + 1], 0.0)
        work = work - column * scaled_row
    on_diag = jnp.where(lanes == rows, work, 0.0)
    pivots = jnp.sqrt(jnp.sum(on_diag, axis=1, keepdims=True))
    diag_row = jnp.sqrt(jnp.sum(on_diag, axis=0, keepdims=True))[:, :size]
    return work[:, size:] / pivots, diag_row


def factor_body(days, core_ref, mine_ref, theirs_ref, inv_ref, diag_ref, full_ref):
    joined(core_ref, mine_ref, theirs_ref, full_ref)
    size = inv_ref.shape[0]
    inverse, diag_row = eliminate(full_ref[:, days : days + size])
    inv_ref[...] = inverse
    diag_ref[...] = diag_row


def last_gram_body(days_all, scaled, par_ref, mine_ref, theirs_ref, inv_ref, applied_ref, gram_ref, full_ref):
    joined(par_ref, mine_ref, theirs_ref, full_ref)
    applied = jnp.dot(inv_ref[...], full_ref[...] / days_all, precision=HIGH, preferred_element_type=F32)
    applied_ref[...] = applied
    gram_ref[...] = gram_of(applied)


def last_body(scale, applied_ref, gram_ref, out_ref, diag_ref):
    inverse, diag_row = eliminate(gram_ref[...])
    vectors = jnp.dot(inverse, applied_ref[...], precision=HIGH, preferred_element_type=F32)
    out_ref[...] = (vectors * scale).T
    diag_ref[...] = diag_row


def swap(x, axis, mask):
    size = lax.axis_size(axis)
    return lax.ppermute(x, axis, [(s, s ^ mask) for s in range(size)])


def tree(parts):
    while len(parts) > 1:
        parts = [parts[i] + parts[i + 1] for i in range(0, len(parts), 2)]
    return parts[0]


def sum_chips(x):
    size = lax.axis_size("gr")
    return tree([x if m == 0 else swap(x, "gr", m) for m in range(0, size, 2)])


def sum_days(keep, send):
    size = lax.axis_size("gc")
    mine = keep + swap(send, "gc", 1)
    mask = 2
    while mask < size:
        mine = mine + swap(mine, "gc", mask)
        mask *= 2
    return mine, swap(mine, "gc", 1)


def sum_assets(keep, send):
    mine = sum_chips(keep + swap(send, "gr", 1))
    return mine, swap(mine, "gr", 1)


def local(returns, start_seed):
    days, assets = returns.shape
    factors = start_seed.shape[1]
    blocks, slabs = lax.axis_size("gr"), lax.axis_size("gc")
    span = assets // blocks
    slab_days = days * blocks
    days_all = slab_days * slabs
    core = (lax.axis_index("gr") % 2).astype(jnp.int32).reshape(1)
    par = (lax.axis_index("gc") % 2).astype(jnp.int32).reshape(1)
    wide = span + -(-3 * factors // LANES) * LANES
    half = factors // 2
    packed_width = slab_days + LANES
    dots = 6 * factors * slab_days * span

    (sent,) = call(first_body, [((blocks, days, wide), BF16)], [], [returns, start_seed], 4 * days * assets * factors)
    block = lax.all_to_all(sent, "gr", 0, 0).reshape(slab_days, wide)
    asset_half = ((half, span), F32)
    day_half = ((half, packed_width), F32)
    full_assets = pltpu.VMEM((factors, span), F32)
    full_days = pltpu.VMEM((factors, packed_width), F32)

    keep, send = call(
        functools.partial(apply_first_body, span), [asset_half] * 2, [par], [block], dots, [full_assets]
    )
    inverse = None
    diagonals = []
    for sweep in range(ITERS - 1):
        mine, theirs = sum_days(keep, send)
        arrays = [mine, theirs, block] + ([] if inverse is None else [inverse])
        keep, send = call(
            functools.partial(project_body, days_all, inverse is not None, span),
            [day_half] * 2, [par, core], arrays, dots, [full_assets, full_days],
        )
        mine, theirs = sum_assets(keep, send)
        keep, send = call(
            functools.partial(apply_body, span), [asset_half] * 2, [core, par], [mine, theirs, block],
            dots, [full_days, full_assets],
        )
        inverse, diag_row = call(
            functools.partial(factor_body, slab_days),
            [((factors, factors), F32), ((1, factors), F32)], [core], [mine, theirs],
            dots, [full_days],
        )
        diagonals.append(diag_row)
    mine, theirs = sum_days(keep, send)
    applied, gram = call(
        functools.partial(last_gram_body, days_all, True),
        [((factors, span), F32), ((factors, factors), F32)], [par], [mine, theirs, inverse],
        dots, [full_assets],
    )
    gram = sum_chips(gram + swap(gram, "gr", 1))
    loadings, diag_row = call(
        functools.partial(last_body, math.sqrt(assets)),
        [((span, factors), F32), ((1, factors), F32)], [], [applied, gram], dots,
    )
    diagonals.append(diag_row)
    return loadings, jnp.concatenate(diagonals, axis=0)


def solution(mesh):
    placed = (P(("gr", "gc"), None), P())
    return jax.shard_map(
        local, mesh=mesh, in_specs=placed, out_specs=(P("gr", None), P()), check_vma=False
    )
```

```python
import functools
import math

import jax
import jax.numpy as jnp
from jax import lax
from jax.experimental import pallas as pl
from jax.experimental.pallas import tpu as pltpu
from jax.sharding import PartitionSpec as P

ITERS = 3
LANES = 128
GROUP = 8
HIGH = lax.Precision.HIGHEST
F32 = jnp.float32
BF16 = jnp.bfloat16


def vmem(count):
    return [pl.BlockSpec(memory_space=pltpu.VMEM)] * count


def smem():
    return [pl.BlockSpec(memory_space=pltpu.SMEM)]


def call(body, outs, scalars, arrays, flops, scratch=()):
    in_specs = smem() * len(scalars) + vmem(len(arrays))
    moved = sum(math.prod(o[0]) * 4 for o in outs)
    return pl.pallas_call(
        body,
        out_shape=[jax.ShapeDtypeStruct(shape, dtype) for shape, dtype in outs],
        in_specs=in_specs,
        out_specs=vmem(len(outs)),
        scratch_shapes=list(scratch),
        cost_estimate=pl.CostEstimate(flops=flops, bytes_accessed=moved, transcendentals=0),
        compiler_params=pltpu.CompilerParams(vmem_limit_bytes=40 * 1024 * 1024),
    )(*scalars, *arrays)


def thirds(x):
    top = x.astype(BF16)
    rest = x - top.astype(F32)
    mid = rest.astype(BF16)
    low = (rest - mid.astype(F32)).astype(BF16)
    return top, mid, low


def fold(tall, rows):
    return tall[2 * rows :] + tall[rows : 2 * rows] + tall[:rows]


def widths(x_ref, blocks, span):
    return [x_ref[:, pl.ds(b * span, span)] for b in range(blocks)]


def project_first_body(returns_ref, seed_ref, out_ref):
    factors = out_ref.shape[0]
    seed = seed_ref[...]
    coarse = (seed >> 3) << 3
    fine = seed - coarse
    both = jnp.concatenate([coarse.astype(F32).astype(BF16), fine.astype(F32).astype(BF16)], axis=0)
    tall = lax.dot_general(both, returns_ref[...], (((1,), (1,)), ((), ())), preferred_element_type=F32)
    out_ref[...] = (tall[:factors] + tall[factors:]) / 1000.0


def deal_body(returns_ref, out_ref):
    out_ref[0] = returns_ref[...]


def deal(returns, blocks):
    days, assets = returns.shape
    span = assets // blocks
    return pl.pallas_call(
        deal_body,
        grid=(blocks,),
        out_shape=jax.ShapeDtypeStruct((blocks, days, span), returns.dtype),
        in_specs=[pl.BlockSpec((days, span), lambda b: (0, b))],
        out_specs=pl.BlockSpec((1, days, span), lambda b: (b, 0, 0)),
    )(returns)


def halves(par_ref, full_ref, keep_ref, send_ref):
    rows = keep_ref.shape[0]
    at = pl.multiple_of(par_ref[0] * rows, 8)
    other = pl.multiple_of((1 - par_ref[0]) * rows, 8)
    keep_ref[...] = full_ref[pl.ds(at, rows), :]
    send_ref[...] = full_ref[pl.ds(other, rows), :]


def joined(par_ref, mine_ref, theirs_ref, full_ref):
    rows = mine_ref.shape[0]
    at = pl.multiple_of(par_ref[0] * rows, 8)
    other = pl.multiple_of((1 - par_ref[0]) * rows, 8)
    full_ref[pl.ds(at, rows), :] = mine_ref[...]
    full_ref[pl.ds(other, rows), :] = theirs_ref[...]


def lane_halves(par_ref, full_ref, keep_ref, send_ref):
    lanes = keep_ref.shape[1]
    at = pl.multiple_of(par_ref[0] * lanes, LANES)
    other = pl.multiple_of((1 - par_ref[0]) * lanes, LANES)
    keep_ref[...] = full_ref[:, pl.ds(at, lanes)]
    send_ref[...] = full_ref[:, pl.ds(other, lanes)]


def lane_joined(par_ref, mine_ref, theirs_ref, full_ref):
    lanes = mine_ref.shape[1]
    at = pl.multiple_of(par_ref[0] * lanes, LANES)
    other = pl.multiple_of((1 - par_ref[0]) * lanes, LANES)
    full_ref[:, pl.ds(at, lanes)] = mine_ref[...]
    full_ref[:, pl.ds(other, lanes)] = theirs_ref[...]


def back_project(projected, block_ref):
    parts = jnp.concatenate(thirds(projected), axis=0)
    tall = jnp.dot(parts, block_ref[...], preferred_element_type=F32)
    return fold(tall, projected.shape[0])


def apply_first_body(masks, me_ref, par_ref, own_ref, twin_ref, *rest):
    pairs = rest[: len(masks)]
    block_ref, keep_ref, send_ref, proj_ref, full_ref = rest[len(masks) :]
    days = own_ref.shape[1]
    me = me_ref[0]

    def place(source, value):
        proj_ref[:, pl.ds(pl.multiple_of(source * days, LANES), days)] = value

    place(me, own_ref[...])
    place(me ^ 1, twin_ref[...])
    for mask, pair_ref in zip(masks, pairs):
        place(me ^ mask, pair_ref[0])
        place(me ^ mask ^ 1, pair_ref[1])
    full_ref[...] = back_project(proj_ref[...], block_ref)
    lane_halves(par_ref, full_ref, keep_ref, send_ref)


def apply_body(core_ref, par_ref, mine_ref, theirs_ref, block_ref, keep_ref, send_ref, proj_ref, full_ref):
    joined(core_ref, mine_ref, theirs_ref, proj_ref)
    full_ref[...] = back_project(proj_ref[:, : block_ref.shape[0]], block_ref)
    lane_halves(par_ref, full_ref, keep_ref, send_ref)


def gram_of(applied):
    return lax.dot_general(applied, applied, (((1,), (1,)), ((), ())), precision=HIGH, preferred_element_type=F32)


def project_body(days_all, scaled, par_ref, core_ref, mine_ref, theirs_ref, block_ref, *rest):
    if scaled:
        inv_ref, keep_ref, send_ref, full_ref, out_ref = rest
    else:
        keep_ref, send_ref, full_ref, out_ref = rest
    lane_joined(par_ref, mine_ref, theirs_ref, full_ref)
    factors = full_ref.shape[0]
    applied = full_ref[...] / days_all
    if scaled:
        applied = jnp.dot(inv_ref[...], applied, precision=HIGH, preferred_element_type=F32)
    days = block_ref.shape[0]
    parts = jnp.concatenate(thirds(applied), axis=0)
    tall = lax.dot_general(parts, block_ref[...], (((1,), (1,)), ((), ())), preferred_element_type=F32)
    out_ref[:, :days] = fold(tall, factors)
    out_ref[:, days:] = jnp.concatenate(
        [gram_of(applied), jnp.zeros((factors, out_ref.shape[1] - days - factors), F32)], axis=1
    )
    halves(core_ref, out_ref, keep_ref, send_ref)


def eliminate(gram):
    size = gram.shape[0]
    rows = lax.broadcasted_iota(jnp.int32, (size, 2 * size), 0)
    lanes = lax.broadcasted_iota(jnp.int32, (size, 2 * size), 1)
    work = jnp.concatenate([gram, jnp.zeros_like(gram)], axis=1)
    work = jnp.where(lanes == rows + size, 1.0, work)
    for first in range(0, size, GROUP):
        columns = [jnp.broadcast_to(work[:, first + j : first + j + 1], work.shape) for j in range(GROUP)]
        for j in range(GROUP):
            k = first + j
            inverse = 1.0 / columns[j][k : k + 1, :]
            below = jnp.where(rows > k, columns[j], 0.0)
            for later in range(j + 1, GROUP):
                columns[later] = columns[later] - below * (columns[later][k : k + 1, :] * inverse)
            work = work - below * (work[k : k + 1, :] * inverse)
    on_diag = jnp.where(lanes == rows, work, 0.0)
    pivots = jnp.sqrt(jnp.sum(on_diag, axis=1, keepdims=True))
    diag_row = jnp.sqrt(jnp.sum(on_diag, axis=0, keepdims=True))[:, :size]
    return work[:, size:] / pivots, diag_row


def factor_body(days, core_ref, mine_ref, theirs_ref, inv_ref, diag_ref, full_ref):
    joined(core_ref, mine_ref, theirs_ref, full_ref)
    size = inv_ref.shape[0]
    inverse, diag_row = eliminate(full_ref[:, days : days + size])
    inv_ref[...] = inverse
    diag_ref[...] = diag_row


def last_gram_body(days_all, mine_ref, inv_ref, gram_ref):
    applied = jnp.dot(inv_ref[...], mine_ref[...] / days_all, precision=HIGH, preferred_element_type=F32)
    gram_ref[...] = gram_of(applied)


def last_body(scale, days_all, par_ref, mine_ref, theirs_ref, inv_ref, gram_ref, *rest):
    diag_refs = rest[: ITERS - 1]
    out_ref, strengths_ref, full_ref = rest[ITERS - 1 :]
    lane_joined(par_ref, mine_ref, theirs_ref, full_ref)
    applied = jnp.dot(inv_ref[...], full_ref[...] / days_all, precision=HIGH, preferred_element_type=F32)
    inverse, diag_row = eliminate(gram_ref[...])
    out_ref[...] = jnp.dot(inverse, applied, precision=HIGH, preferred_element_type=F32) * scale
    for k, ref in enumerate(diag_refs):
        strengths_ref[k : k + 1, :] = ref[...]
    strengths_ref[ITERS - 1 : ITERS, :] = diag_row


def swap(x, axis, mask):
    size = lax.axis_size(axis)
    return lax.ppermute(x, axis, [(s, s ^ mask) for s in range(size)])


def tree(parts):
    while len(parts) > 1:
        parts = [parts[i] + parts[i + 1] for i in range(0, len(parts), 2)]
    return parts[0]


def sum_chips(x):
    size = lax.axis_size("gr")
    return tree([x if m == 0 else swap(x, "gr", m) for m in range(0, size, 2)])


def sum_days(keep, send):
    size = lax.axis_size("gc")
    mine = keep + swap(send, "gc", 1)
    mask = 2
    while mask < size:
        mine = mine + swap(mine, "gc", mask)
        mask *= 2
    return mine


def sum_assets(keep, send):
    mine = sum_chips(keep + swap(send, "gr", 1))
    return mine, swap(mine, "gr", 1)


def local(returns, start_seed):
    days, assets = returns.shape
    factors = start_seed.shape[1]
    blocks, slabs = lax.axis_size("gr"), lax.axis_size("gc")
    span = assets // blocks
    slab_days = days * blocks
    days_all = slab_days * slabs
    core = (lax.axis_index("gr") % 2).astype(jnp.int32).reshape(1)
    par = (lax.axis_index("gc") % 2).astype(jnp.int32).reshape(1)
    me = lax.axis_index("gr").astype(jnp.int32).reshape(1)
    half = factors // 2
    packed_width = slab_days + LANES
    dots = 6 * factors * slab_days * span

    block = lax.all_to_all(deal(returns, blocks), "gr", 0, 0).reshape(slab_days, span)
    (own,) = call(
        project_first_body, [((factors, days), F32)], [], [returns, start_seed.T], 4 * days * assets * factors
    )
    twin = swap(own, "gr", 1)
    both = jnp.stack([own, twin])
    masks = tuple(range(2, blocks, 2))
    pairs = [swap(both, "gr", m) for m in masks]

    asset_half = ((factors, span // 2), F32)
    day_half = ((half, packed_width), F32)
    full_assets = pltpu.VMEM((factors, span), F32)
    slab = pltpu.VMEM((factors, slab_days), F32)
    full_days = pltpu.VMEM((factors, packed_width), F32)

    keep, send = call(
        functools.partial(apply_first_body, masks), [asset_half] * 2, [me, par],
        [own, twin, *pairs, block], dots, [slab, full_assets],
    )
    inverse = None
    diagonals = []
    for sweep in range(ITERS - 1):
        mine = sum_days(keep, send)
        theirs = swap(mine, "gc", 1)
        arrays = [mine, theirs, block] + ([] if inverse is None else [inverse])
        keep, send = call(
            functools.partial(project_body, days_all, inverse is not None),
            [day_half] * 2, [par, core], arrays, dots, [full_assets, full_days],
        )
        mine, theirs = sum_assets(keep, send)
        keep, send = call(
            apply_body, [asset_half] * 2, [core, par], [mine, theirs, block], dots, [full_days, full_assets]
        )
        inverse, diag_row = call(
            functools.partial(factor_body, slab_days),
            [((factors, factors), F32), ((1, factors), F32)], [core], [mine, theirs],
            dots, [full_days],
        )
        diagonals.append(diag_row)
    mine = sum_days(keep, send)
    (gram,) = call(
        functools.partial(last_gram_body, days_all), [((factors, factors), F32)], [], [mine, inverse], dots
    )
    gram = gram + swap(gram, "gr", 1)
    gram = gram + swap(gram, "gc", 1)
    theirs = swap(mine, "gc", 1)
    gram = sum_chips(gram)
    loadings, strengths = call(
        functools.partial(last_body, math.sqrt(assets), days_all),
        [((factors, span), F32), ((ITERS, factors), F32)], [par],
        [mine, theirs, inverse, gram, *diagonals], dots, [full_assets],
    )
    return loadings.T, strengths


def solution(mesh):
    placed = (P(("gr", "gc"), None), P())
    return jax.shard_map(
        local, mesh=mesh, in_specs=placed, out_specs=(P("gr", None), P()), check_vma=False
    )
```

```python
import functools
import math

import jax
import jax.numpy as jnp
from jax import lax
from jax.experimental import pallas as pl
from jax.experimental.pallas import tpu as pltpu
from jax.sharding import PartitionSpec as P

ITERS = 3
LANES = 128
GROUP = 8
HIGH = lax.Precision.HIGHEST
F32 = jnp.float32
BF16 = jnp.bfloat16


def vmem(count):
    return [pl.BlockSpec(memory_space=pltpu.VMEM)] * count


def smem():
    return [pl.BlockSpec(memory_space=pltpu.SMEM)]


def call(body, outs, scalars, arrays, flops, scratch=()):
    in_specs = smem() * len(scalars) + vmem(len(arrays))
    moved = sum(math.prod(o[0]) * 4 for o in outs)
    return pl.pallas_call(
        body,
        out_shape=[jax.ShapeDtypeStruct(shape, dtype) for shape, dtype in outs],
        in_specs=in_specs,
        out_specs=vmem(len(outs)),
        scratch_shapes=list(scratch),
        cost_estimate=pl.CostEstimate(flops=flops, bytes_accessed=moved, transcendentals=0),
        compiler_params=pltpu.CompilerParams(vmem_limit_bytes=40 * 1024 * 1024),
    )(*scalars, *arrays)


def thirds(x):
    top = x.astype(BF16)
    rest = x - top.astype(F32)
    mid = rest.astype(BF16)
    low = (rest - mid.astype(F32)).astype(BF16)
    return top, mid, low


def fold(tall, rows):
    return tall[2 * rows :] + tall[rows : 2 * rows] + tall[:rows]


def widths(x_ref, blocks, span):
    return [x_ref[:, pl.ds(b * span, span)] for b in range(blocks)]


def project_first_body(returns_ref, seed_ref, out_ref):
    factors = out_ref.shape[0]
    seed = seed_ref[...]
    coarse = (seed >> 3) << 3
    fine = seed - coarse
    both = jnp.concatenate([coarse.astype(F32).astype(BF16), fine.astype(F32).astype(BF16)], axis=0)
    tall = lax.dot_general(both, returns_ref[...], (((1,), (1,)), ((), ())), preferred_element_type=F32)
    out_ref[...] = (tall[:factors] + tall[factors:]) / 1000.0


def halves(par_ref, full_ref, keep_ref, send_ref):
    rows = keep_ref.shape[0]
    at = pl.multiple_of(par_ref[0] * rows, 8)
    other = pl.multiple_of((1 - par_ref[0]) * rows, 8)
    keep_ref[...] = full_ref[pl.ds(at, rows), :]
    send_ref[...] = full_ref[pl.ds(other, rows), :]


def joined(par_ref, mine_ref, theirs_ref, full_ref):
    rows = mine_ref.shape[0]
    at = pl.multiple_of(par_ref[0] * rows, 8)
    other = pl.multiple_of((1 - par_ref[0]) * rows, 8)
    full_ref[pl.ds(at, rows), :] = mine_ref[...]
    full_ref[pl.ds(other, rows), :] = theirs_ref[...]


def lane_halves(par_ref, full_ref, keep_ref, send_ref):
    lanes = keep_ref.shape[1]
    at = pl.multiple_of(par_ref[0] * lanes, LANES)
    other = pl.multiple_of((1 - par_ref[0]) * lanes, LANES)
    keep_ref[...] = full_ref[:, pl.ds(at, lanes)]
    send_ref[...] = full_ref[:, pl.ds(other, lanes)]


def lane_joined(par_ref, mine_ref, theirs_ref, full_ref):
    lanes = mine_ref.shape[1]
    at = pl.multiple_of(par_ref[0] * lanes, LANES)
    other = pl.multiple_of((1 - par_ref[0]) * lanes, LANES)
    full_ref[:, pl.ds(at, lanes)] = mine_ref[...]
    full_ref[:, pl.ds(other, lanes)] = theirs_ref[...]


def back_project(projected, block_ref):
    parts = jnp.concatenate(thirds(projected), axis=0)
    tall = jnp.dot(parts, block_ref[...], preferred_element_type=F32)
    return fold(tall, projected.shape[0])


def apply_first_body(masks, me_ref, par_ref, own_ref, twin_ref, *rest):
    pairs = rest[: len(masks)]
    block_ref, keep_ref, send_ref, proj_ref, full_ref = rest[len(masks) :]
    days = own_ref.shape[1]
    me = me_ref[0]

    def place(source, value):
        proj_ref[:, pl.ds(pl.multiple_of(source * days, LANES), days)] = value

    place(me, own_ref[...])
    place(me ^ 1, twin_ref[...])
    for mask, pair_ref in zip(masks, pairs):
        place(me ^ mask, pair_ref[0])
        place(me ^ mask ^ 1, pair_ref[1])
    full_ref[...] = back_project(proj_ref[...], block_ref)
    lane_halves(par_ref, full_ref, keep_ref, send_ref)


def apply_body(core_ref, par_ref, mine_ref, theirs_ref, block_ref, keep_ref, send_ref, proj_ref, full_ref):
    joined(core_ref, mine_ref, theirs_ref, proj_ref)
    full_ref[...] = back_project(proj_ref[:, : block_ref.shape[0]], block_ref)
    lane_halves(par_ref, full_ref, keep_ref, send_ref)


def gram_of(applied):
    return lax.dot_general(applied, applied, (((1,), (1,)), ((), ())), precision=HIGH, preferred_element_type=F32)


def project_body(days_all, scaled, par_ref, core_ref, mine_ref, theirs_ref, block_ref, *rest):
    if scaled:
        inv_ref, keep_ref, send_ref, full_ref, out_ref = rest
    else:
        keep_ref, send_ref, full_ref, out_ref = rest
    lane_joined(par_ref, mine_ref, theirs_ref, full_ref)
    factors = full_ref.shape[0]
    applied = full_ref[...] / days_all
    if scaled:
        applied = jnp.dot(inv_ref[...], applied, precision=HIGH, preferred_element_type=F32)
    days = block_ref.shape[0]
    parts = jnp.concatenate(thirds(applied), axis=0)
    tall = lax.dot_general(parts, block_ref[...], (((1,), (1,)), ((), ())), preferred_element_type=F32)
    out_ref[:, :days] = fold(tall, factors)
    out_ref[:, days:] = jnp.concatenate(
        [gram_of(applied), jnp.zeros((factors, out_ref.shape[1] - days - factors), F32)], axis=1
    )
    halves(core_ref, out_ref, keep_ref, send_ref)


def eliminate(gram):
    size = gram.shape[0]
    rows = lax.broadcasted_iota(jnp.int32, (size, 2 * size), 0)
    lanes = lax.broadcasted_iota(jnp.int32, (size, 2 * size), 1)
    work = jnp.concatenate([gram, jnp.zeros_like(gram)], axis=1)
    work = jnp.where(lanes == rows + size, 1.0, work)
    for first in range(0, size, GROUP):
        columns = [jnp.broadcast_to(work[:, first + j : first + j + 1], work.shape) for j in range(GROUP)]
        for j in range(GROUP):
            k = first + j
            inverse = 1.0 / columns[j][k : k + 1, :]
            below = jnp.where(rows > k, columns[j], 0.0)
            for later in range(j + 1, GROUP):
                columns[later] = columns[later] - below * (columns[later][k : k + 1, :] * inverse)
            work = work - below * (work[k : k + 1, :] * inverse)
    on_diag = jnp.where(lanes == rows, work, 0.0)
    pivots = jnp.sqrt(jnp.sum(on_diag, axis=1, keepdims=True))
    diag_row = jnp.sqrt(jnp.sum(on_diag, axis=0, keepdims=True))[:, :size]
    return work[:, size:] / pivots, diag_row


def factor_body(days, core_ref, mine_ref, theirs_ref, inv_ref, diag_ref, full_ref):
    joined(core_ref, mine_ref, theirs_ref, full_ref)
    size = inv_ref.shape[0]
    inverse, diag_row = eliminate(full_ref[:, days : days + size])
    inv_ref[...] = inverse
    diag_ref[...] = diag_row


def last_gram_body(days_all, mine_ref, inv_ref, applied_ref, gram_ref):
    applied = jnp.dot(inv_ref[...], mine_ref[...] / days_all, precision=HIGH, preferred_element_type=F32)
    applied_ref[...] = applied
    gram = gram_of(applied)
    half = gram_ref.shape[0]
    gram_ref[...] = jnp.concatenate([gram[:half], gram[half:]], axis=1)


def last_body(scale, par_ref, mine_ref, theirs_ref, gram_ref, *rest):
    diag_refs = rest[: ITERS - 1]
    out_ref, strengths_ref, full_ref = rest[ITERS - 1 :]
    lane_joined(par_ref, mine_ref, theirs_ref, full_ref)
    factors = full_ref.shape[0]
    gram = jnp.concatenate([gram_ref[:, :factors], gram_ref[:, factors:]], axis=0)
    inverse, diag_row = eliminate(gram)
    out_ref[...] = jnp.dot(inverse, full_ref[...], precision=HIGH, preferred_element_type=F32) * scale
    for k, ref in enumerate(diag_refs):
        strengths_ref[k : k + 1, :] = ref[...]
    strengths_ref[ITERS - 1 : ITERS, :] = diag_row


def swap(x, axis, mask):
    size = lax.axis_size(axis)
    return lax.ppermute(x, axis, [(s, s ^ mask) for s in range(size)])


def tree(parts):
    while len(parts) > 1:
        parts = [parts[i] + parts[i + 1] for i in range(0, len(parts), 2)]
    return parts[0]


def sum_chips(x):
    size = lax.axis_size("gr")
    return tree([x if m == 0 else swap(x, "gr", m) for m in range(0, size, 2)])


def sum_days(keep, send):
    size = lax.axis_size("gc")
    mine = keep + swap(send, "gc", 1)
    mask = 2
    while mask < size:
        mine = mine + swap(mine, "gc", mask)
        mask *= 2
    return mine


def sum_assets(keep, send):
    mine = sum_chips(keep + swap(send, "gr", 1))
    return mine, swap(mine, "gr", 1)


def local(returns, start_seed):
    days, assets = returns.shape
    factors = start_seed.shape[1]
    blocks, slabs = lax.axis_size("gr"), lax.axis_size("gc")
    span = assets // blocks
    slab_days = days * blocks
    days_all = slab_days * slabs
    core = (lax.axis_index("gr") % 2).astype(jnp.int32).reshape(1)
    par = (lax.axis_index("gc") % 2).astype(jnp.int32).reshape(1)
    me = lax.axis_index("gr").astype(jnp.int32).reshape(1)
    half = factors // 2
    packed_width = slab_days + LANES
    dots = 6 * factors * slab_days * span

    block = lax.all_to_all(returns, "gr", 1, 0, tiled=True)
    (own,) = call(
        project_first_body, [((factors, days), F32)], [], [returns, start_seed.T], 4 * days * assets * factors
    )
    twin = swap(own, "gr", 1)
    both = jnp.stack([own, twin])
    masks = tuple(range(2, blocks, 2))
    pairs = [swap(both, "gr", m) for m in masks]

    asset_half = ((factors, span // 2), F32)
    day_half = ((half, packed_width), F32)
    full_assets = pltpu.VMEM((factors, span), F32)
    slab = pltpu.VMEM((factors, slab_days), F32)
    full_days = pltpu.VMEM((factors, packed_width), F32)

    keep, send = call(
        functools.partial(apply_first_body, masks), [asset_half] * 2, [me, par],
        [own, twin, *pairs, block], dots, [slab, full_assets],
    )
    inverse = None
    diagonals = []
    for sweep in range(ITERS - 1):
        mine = sum_days(keep, send)
        theirs = swap(mine, "gc", 1)
        arrays = [mine, theirs, block] + ([] if inverse is None else [inverse])
        keep, send = call(
            functools.partial(project_body, days_all, inverse is not None),
            [day_half] * 2, [par, core], arrays, dots, [full_assets, full_days],
        )
        mine, theirs = sum_assets(keep, send)
        keep, send = call(
            apply_body, [asset_half] * 2, [core, par], [mine, theirs, block], dots, [full_days, full_assets]
        )
        inverse, diag_row = call(
            functools.partial(factor_body, slab_days),
            [((factors, factors), F32), ((1, factors), F32)], [core], [mine, theirs],
            dots, [full_days],
        )
        diagonals.append(diag_row)
    mine = sum_days(keep, send)
    applied, gram = call(
        functools.partial(last_gram_body, days_all),
        [asset_half, ((half, 2 * factors), F32)], [], [mine, inverse], dots,
    )
    theirs = swap(applied, "gc", 1)
    gram = sum_chips(gram + swap(gram, "gr", 1))
    gram, theirs = lax.optimization_barrier((gram, theirs))
    gram = gram + swap(gram, "gc", 1)
    loadings, strengths = call(
        functools.partial(last_body, math.sqrt(assets)),
        [((factors, span), F32), ((ITERS, factors), F32)], [par],
        [applied, theirs, gram, *diagonals], dots, [full_assets],
    )
    return loadings.T, strengths


def solution(mesh):
    placed = (P(("gr", "gc"), None), P())
    return jax.shard_map(
        local, mesh=mesh, in_specs=placed, out_specs=(P("gr", None), P()), check_vma=False
    )
```

```python
import functools
import math

import jax
import jax.numpy as jnp
from jax import lax
from jax.experimental import pallas as pl
from jax.experimental.pallas import tpu as pltpu
from jax.sharding import PartitionSpec as P

ITERS = 3
LANES = 128
GROUP = 8
CUT = 4
HIGH = lax.Precision.HIGHEST
F32 = jnp.float32
BF16 = jnp.bfloat16


def vmem(count):
    return [pl.BlockSpec(memory_space=pltpu.VMEM)] * count


def smem():
    return [pl.BlockSpec(memory_space=pltpu.SMEM)]


def call(body, outs, scalars, arrays, flops, scratch=()):
    in_specs = smem() * len(scalars) + vmem(len(arrays))
    moved = sum(math.prod(o[0]) * 4 for o in outs)
    return pl.pallas_call(
        body,
        out_shape=[jax.ShapeDtypeStruct(shape, dtype) for shape, dtype in outs],
        in_specs=in_specs,
        out_specs=vmem(len(outs)),
        scratch_shapes=list(scratch),
        cost_estimate=pl.CostEstimate(flops=flops, bytes_accessed=moved, transcendentals=0),
        compiler_params=pltpu.CompilerParams(vmem_limit_bytes=40 * 1024 * 1024),
    )(*scalars, *arrays)


def thirds(x):
    top = x.astype(BF16)
    rest = x - top.astype(F32)
    mid = rest.astype(BF16)
    low = (rest - mid.astype(F32)).astype(BF16)
    return top, mid, low


def fold(tall, rows):
    return tall[2 * rows :] + tall[rows : 2 * rows] + tall[:rows]


def deal_body(returns_ref, out_ref, sems):
    blocks, _, width = out_ref.shape
    span = returns_ref.shape[1] // blocks
    copies = [
        pltpu.make_async_copy(returns_ref.at[:, b * span : b * span + width], out_ref.at[b], sems.at[b])
        for b in range(blocks)
    ]
    for copy in copies:
        copy.start()
    for copy in copies:
        copy.wait()


def deal(returns, blocks, width):
    return pl.pallas_call(
        deal_body,
        out_shape=jax.ShapeDtypeStruct((blocks, returns.shape[0], width), returns.dtype),
        in_specs=[pl.BlockSpec(memory_space=pl.ANY)],
        out_specs=pl.BlockSpec(memory_space=pltpu.VMEM),
        scratch_shapes=[pltpu.SemaphoreType.DMA((blocks,))],
    )(returns)


def project_first_body(span, me_ref, returns_ref, seed_ref, out_ref, *pieces):
    factors = out_ref.shape[0]
    for mask, piece in enumerate(pieces):
        width = piece.shape[1]
        at = pl.multiple_of((me_ref[0] ^ mask) * span + span - width, LANES)
        piece[...] = returns_ref[:, pl.ds(at, width)]
    seed = seed_ref[...]
    coarse = (seed >> 3) << 3
    fine = seed - coarse
    both = jnp.concatenate([coarse.astype(F32).astype(BF16), fine.astype(F32).astype(BF16)], axis=0)
    tall = lax.dot_general(both, returns_ref[...], (((1,), (1,)), ((), ())), preferred_element_type=F32)
    out_ref[...] = (tall[:factors] + tall[factors:]) / 1000.0


def halves(par_ref, full_ref, keep_ref, send_ref):
    rows = keep_ref.shape[0]
    at = pl.multiple_of(par_ref[0] * rows, 8)
    other = pl.multiple_of((1 - par_ref[0]) * rows, 8)
    keep_ref[...] = full_ref[pl.ds(at, rows), :]
    send_ref[...] = full_ref[pl.ds(other, rows), :]


def joined(par_ref, mine_ref, theirs_ref, full_ref):
    rows = mine_ref.shape[0]
    at = pl.multiple_of(par_ref[0] * rows, 8)
    other = pl.multiple_of((1 - par_ref[0]) * rows, 8)
    full_ref[pl.ds(at, rows), :] = mine_ref[...]
    full_ref[pl.ds(other, rows), :] = theirs_ref[...]


def lane_halves(par_ref, full_ref, keep_ref, send_ref):
    lanes = keep_ref.shape[1]
    at = pl.multiple_of(par_ref[0] * lanes, LANES)
    other = pl.multiple_of((1 - par_ref[0]) * lanes, LANES)
    keep_ref[...] = full_ref[:, pl.ds(at, lanes)]
    send_ref[...] = full_ref[:, pl.ds(other, lanes)]


def lane_joined(par_ref, mine_ref, theirs_ref, full_ref, start=0):
    lanes = mine_ref.shape[1]
    at = pl.multiple_of(start + par_ref[0] * lanes, LANES)
    other = pl.multiple_of(start + (1 - par_ref[0]) * lanes, LANES)
    full_ref[:, pl.ds(at, lanes)] = mine_ref[...]
    full_ref[:, pl.ds(other, lanes)] = theirs_ref[...]


def spans(block_refs):
    start, found = 0, []
    for ref in block_refs:
        found.append((start, ref))
        start += ref.shape[1]
    return found


def back_project(projected, block_refs, full_ref):
    parts = jnp.concatenate(thirds(projected), axis=0)
    for start, ref in spans(block_refs):
        tall = jnp.dot(parts, ref[...], preferred_element_type=F32)
        full_ref[:, start : start + ref.shape[1]] = fold(tall, projected.shape[0])


def forward_project(applied, block_refs):
    total = 0.0
    for start, ref in spans(block_refs):
        parts = jnp.concatenate(thirds(applied[:, start : start + ref.shape[1]]), axis=0)
        tall = lax.dot_general(parts, ref[...], (((1,), (1,)), ((), ())), preferred_element_type=F32)
        total = total + fold(tall, applied.shape[0])
    return total


def apply_first_body(masks, gathered, me_ref, par_ref, own_ref, twin_ref, *rest):
    pairs = rest[: len(masks)]
    rest = rest[len(masks) :]
    me = me_ref[0]
    days = own_ref.shape[1]
    if gathered:
        *pieces, block_ref, keep_ref, send_ref, proj_ref, full_ref = rest
        for mask, piece in enumerate(pieces):
            block_ref[pl.ds(pl.multiple_of((me ^ mask) * days, LANES), days), :] = piece[...]
    else:
        block_ref, keep_ref, send_ref, proj_ref, full_ref = rest

    def place(source, value):
        proj_ref[:, pl.ds(pl.multiple_of(source * days, LANES), days)] = value

    place(me, own_ref[...])
    place(me ^ 1, twin_ref[...])
    for mask, pair_ref in zip(masks, pairs):
        place(me ^ mask, pair_ref[0])
        place(me ^ mask ^ 1, pair_ref[1])
    back_project(proj_ref[...], [block_ref], full_ref)
    lane_halves(par_ref, full_ref, keep_ref, send_ref)


def apply_body(core_ref, par_ref, mine_ref, theirs_ref, *rest):
    *block_refs, keep_ref, send_ref, proj_ref, full_ref = rest
    joined(core_ref, mine_ref, theirs_ref, proj_ref)
    back_project(proj_ref[:, : block_refs[0].shape[0]], block_refs, full_ref)
    lane_halves(par_ref, full_ref, keep_ref, send_ref)


def gram_of(applied):
    return lax.dot_general(applied, applied, (((1,), (1,)), ((), ())), precision=HIGH, preferred_element_type=F32)


def project_body(days_all, scaled, pieces, chunks, par_ref, core_ref, *rest):
    halves_refs = rest[: 2 * pieces]
    block_refs = rest[2 * pieces : 2 * pieces + chunks]
    rest = rest[2 * pieces + chunks :]
    inv_ref, rest = (rest[0], rest[1:]) if scaled else (None, rest)
    keep_ref, send_ref, full_ref, out_ref = rest
    start = 0
    for k in range(pieces):
        mine_ref, theirs_ref = halves_refs[2 * k : 2 * k + 2]
        lane_joined(par_ref, mine_ref, theirs_ref, full_ref, start)
        start += 2 * mine_ref.shape[1]
    factors = full_ref.shape[0]
    applied = full_ref[...] / days_all
    if scaled:
        applied = jnp.dot(inv_ref[...], applied, precision=HIGH, preferred_element_type=F32)
    days = block_refs[0].shape[0]
    out_ref[:, :days] = forward_project(applied, block_refs)
    out_ref[:, days:] = jnp.concatenate(
        [gram_of(applied), jnp.zeros((factors, out_ref.shape[1] - days - factors), F32)], axis=1
    )
    halves(core_ref, out_ref, keep_ref, send_ref)


def eliminate(gram):
    size = gram.shape[0]
    rows = lax.broadcasted_iota(jnp.int32, (size, 2 * size), 0)
    lanes = lax.broadcasted_iota(jnp.int32, (size, 2 * size), 1)
    work = jnp.concatenate([gram, jnp.zeros_like(gram)], axis=1)
    work = jnp.where(lanes == rows + size, 1.0, work)
    for first in range(0, size, GROUP):
        columns = [jnp.broadcast_to(work[:, first + j : first + j + 1], work.shape) for j in range(GROUP)]
        for j in range(GROUP):
            k = first + j
            inverse = 1.0 / columns[j][k : k + 1, :]
            below = jnp.where(rows > k, columns[j], 0.0)
            for later in range(j + 1, GROUP):
                columns[later] = columns[later] - below * (columns[later][k : k + 1, :] * inverse)
            work = work - below * (work[k : k + 1, :] * inverse)
    on_diag = jnp.where(lanes == rows, work, 0.0)
    pivots = jnp.sqrt(jnp.sum(on_diag, axis=1, keepdims=True))
    diag_row = jnp.sqrt(jnp.sum(on_diag, axis=0, keepdims=True))[:, :size]
    return work[:, size:] / pivots, diag_row


def factor_body(days, core_ref, mine_ref, theirs_ref, inv_ref, diag_ref, full_ref):
    joined(core_ref, mine_ref, theirs_ref, full_ref)
    size = inv_ref.shape[0]
    inverse, diag_row = eliminate(full_ref[:, days : days + size])
    inv_ref[...] = inverse
    diag_ref[...] = diag_row


def last_gram_body(days_all, mine_ref, inv_ref, applied_ref, gram_ref):
    applied = jnp.dot(inv_ref[...], mine_ref[...] / days_all, precision=HIGH, preferred_element_type=F32)
    applied_ref[...] = applied
    gram = gram_of(applied)
    half = gram_ref.shape[0]
    gram_ref[...] = jnp.concatenate([gram[:half], gram[half:]], axis=1)


def last_body(scale, par_ref, mine_ref, theirs_ref, gram_ref, *rest):
    diag_refs = rest[: ITERS - 1]
    out_ref, strengths_ref, full_ref = rest[ITERS - 1 :]
    lane_joined(par_ref, mine_ref, theirs_ref, full_ref)
    factors = full_ref.shape[0]
    gram = jnp.concatenate([gram_ref[:, :factors], gram_ref[:, factors:]], axis=0)
    inverse, diag_row = eliminate(gram)
    out_ref[...] = jnp.dot(inverse, full_ref[...], precision=HIGH, preferred_element_type=F32) * scale
    for k, ref in enumerate(diag_refs):
        strengths_ref[k : k + 1, :] = ref[...]
    strengths_ref[ITERS - 1 : ITERS, :] = diag_row


def swap(x, axis, mask):
    size = lax.axis_size(axis)
    return lax.ppermute(x, axis, [(s, s ^ mask) for s in range(size)])


def tree(parts):
    while len(parts) > 1:
        parts = [parts[i] + parts[i + 1] for i in range(0, len(parts), 2)]
    return parts[0]


def sum_chips(x):
    size = lax.axis_size("gr")
    return tree([x if m == 0 else swap(x, "gr", m) for m in range(0, size, 2)])


def sum_days(keep, send):
    size = lax.axis_size("gc")
    mine = keep + swap(send, "gc", 1)
    mask = 2
    while mask < size:
        mine = mine + swap(mine, "gc", mask)
        mask *= 2
    return mine


def sum_assets(keep, send):
    mine = sum_chips(keep + swap(send, "gr", 1))
    return mine, swap(mine, "gr", 1)


def local(returns, start_seed):
    days, assets = returns.shape
    factors = start_seed.shape[1]
    blocks, slabs = lax.axis_size("gr"), lax.axis_size("gc")
    span = assets // blocks
    slab_days = days * blocks
    days_all = slab_days * slabs
    core = (lax.axis_index("gr") % 2).astype(jnp.int32).reshape(1)
    par = (lax.axis_index("gc") % 2).astype(jnp.int32).reshape(1)
    me = lax.axis_index("gr").astype(jnp.int32).reshape(1)
    half = factors // 2
    packed_width = slab_days + LANES
    dots = 6 * factors * slab_days * span

    unit = 2 * LANES
    cut = span * CUT // 8 // unit * unit
    rest = span - cut
    masks = tuple(range(2, blocks, 2))

    dealt = deal(returns, blocks, cut)
    block = lax.all_to_all(dealt, "gr", 0, 0).reshape(slab_days, cut)
    own, *pieces = call(
        functools.partial(project_first_body, span),
        [((factors, days), F32)] + [((days, rest), BF16)] * blocks,
        [me], [returns, start_seed.T], 4 * days * assets * factors,
    )
    twin = swap(own, "gr", 1)
    both = jnp.stack([own, twin])
    pairs = [swap(both, "gr", m) for m in masks]
    pieces = [p if m == 0 else swap(p, "gr", m) for m, p in enumerate(pieces)]

    asset_half = ((factors, span // 2), F32)
    day_half = ((half, packed_width), F32)
    full_assets = pltpu.VMEM((factors, span), F32)
    slab = pltpu.VMEM((factors, slab_days), F32)
    full_days = pltpu.VMEM((factors, packed_width), F32)

    shared = [own, twin, *pairs]
    keep, send = call(
        functools.partial(apply_first_body, masks, False), [((factors, cut // 2), F32)] * 2, [me, par],
        shared + [block], dots, [slab, pltpu.VMEM((factors, cut), F32)],
    )
    mine = sum_days(keep, send)
    theirs = swap(mine, "gc", 1)
    last, keep, send = call(
        functools.partial(apply_first_body, masks, True),
        [((slab_days, rest), BF16)] + [((factors, rest // 2), F32)] * 2, [me, par],
        shared + pieces, dots, [slab, pltpu.VMEM((factors, rest), F32)],
    )
    mine_late = sum_days(keep, send)
    pieces = [mine, theirs, mine_late, swap(mine_late, "gc", 1)]
    block_list = [block, last]
    inverse = None
    diagonals = []
    for sweep in range(ITERS - 1):
        if sweep:
            mine = sum_days(keep, send)
            pieces = [mine, swap(mine, "gc", 1)]
        arrays = pieces + block_list + ([] if inverse is None else [inverse])
        keep, send = call(
            functools.partial(
                project_body, days_all, inverse is not None, len(pieces) // 2, len(block_list)
            ),
            [day_half] * 2, [par, core], arrays, dots, [full_assets, full_days],
        )
        mine, theirs = sum_assets(keep, send)
        keep, send = call(
            apply_body, [asset_half] * 2, [core, par], [mine, theirs, *block_list], dots,
            [full_days, full_assets],
        )
        inverse, diag_row = call(
            functools.partial(factor_body, slab_days),
            [((factors, factors), F32), ((1, factors), F32)], [core], [mine, theirs],
            dots, [full_days],
        )
        diagonals.append(diag_row)
    mine = sum_days(keep, send)
    applied, gram = call(
        functools.partial(last_gram_body, days_all),
        [asset_half, ((half, 2 * factors), F32)], [], [mine, inverse], dots,
    )
    theirs = swap(applied, "gc", 1)
    gram = gram + swap(gram, "gr", 1)
    mask = 2
    while mask < blocks:
        gram = gram + swap(gram, "gr", mask)
        mask *= 2
    gram = gram + swap(gram, "gc", 1)
    loadings, strengths = call(
        functools.partial(last_body, math.sqrt(assets)),
        [((factors, span), F32), ((ITERS, factors), F32)], [par],
        [applied, theirs, gram, *diagonals], dots, [full_assets],
    )
    return loadings.T, strengths


def solution(mesh):
    placed = (P(("gr", "gc"), None), P())
    return jax.shard_map(local, mesh=mesh, in_specs=placed, out_specs=(P("gr", None), P()), check_vma=False)
```

```python
import functools
import math

import jax
import jax.numpy as jnp
from jax import lax
from jax.experimental import pallas as pl
from jax.experimental.pallas import tpu as pltpu
from jax.sharding import PartitionSpec as P

ITERS = 3
LANES = 128
GROUP = 8
CUT = 4
HIGH = lax.Precision.HIGHEST
F32 = jnp.float32
BF16 = jnp.bfloat16


def vmem(count):
    return [pl.BlockSpec(memory_space=pltpu.VMEM)] * count


def smem():
    return [pl.BlockSpec(memory_space=pltpu.SMEM)]


def call(body, outs, scalars, arrays, flops, scratch=()):
    in_specs = smem() * len(scalars) + vmem(len(arrays))
    moved = sum(math.prod(o[0]) * 4 for o in outs)
    return pl.pallas_call(
        body,
        out_shape=[jax.ShapeDtypeStruct(shape, dtype) for shape, dtype in outs],
        in_specs=in_specs,
        out_specs=vmem(len(outs)),
        scratch_shapes=list(scratch),
        cost_estimate=pl.CostEstimate(flops=flops, bytes_accessed=moved, transcendentals=0),
        compiler_params=pltpu.CompilerParams(vmem_limit_bytes=16 * 1024 * 1024),
    )(*scalars, *arrays)


def thirds(x):
    top = x.astype(BF16)
    rest = x - top.astype(F32)
    mid = rest.astype(BF16)
    low = (rest - mid.astype(F32)).astype(BF16)
    return top, mid, low


def fold(tall, rows):
    return tall[2 * rows :] + tall[rows : 2 * rows] + tall[:rows]


def deal_body(returns_ref, out_ref, sems):
    blocks, _, width = out_ref.shape
    span = returns_ref.shape[1] // blocks
    copies = [
        pltpu.make_async_copy(returns_ref.at[:, b * span : b * span + width], out_ref.at[b], sems.at[b])
        for b in range(blocks)
    ]
    for copy in copies:
        copy.start()
    for copy in copies:
        copy.wait()


def deal(returns, blocks, width):
    return pl.pallas_call(
        deal_body,
        out_shape=jax.ShapeDtypeStruct((blocks, returns.shape[0], width), returns.dtype),
        in_specs=[pl.BlockSpec(memory_space=pl.ANY)],
        out_specs=pl.BlockSpec(memory_space=pltpu.VMEM),
        scratch_shapes=[pltpu.SemaphoreType.DMA((blocks,))],
    )(returns)


def project_first_body(span, me_ref, returns_ref, seed_ref, out_ref, *pieces):
    factors = out_ref.shape[0]
    for mask, piece in enumerate(pieces):
        width = piece.shape[1]
        at = pl.multiple_of((me_ref[0] ^ mask) * span + span - width, LANES)
        piece[...] = returns_ref[:, pl.ds(at, width)]
    seed = seed_ref[...]
    coarse = (seed >> 3) << 3
    fine = seed - coarse
    both = jnp.concatenate([coarse.astype(F32).astype(BF16), fine.astype(F32).astype(BF16)], axis=0)
    tall = lax.dot_general(both, returns_ref[...], (((1,), (1,)), ((), ())), preferred_element_type=F32)
    out_ref[...] = (tall[:factors] + tall[factors:]) / 1000.0


def halves(par_ref, full_ref, keep_ref, send_ref):
    rows = keep_ref.shape[0]
    at = pl.multiple_of(par_ref[0] * rows, 8)
    other = pl.multiple_of((1 - par_ref[0]) * rows, 8)
    keep_ref[...] = full_ref[pl.ds(at, rows), :]
    send_ref[...] = full_ref[pl.ds(other, rows), :]


def joined(par_ref, mine_ref, theirs_ref, full_ref):
    rows = mine_ref.shape[0]
    at = pl.multiple_of(par_ref[0] * rows, 8)
    other = pl.multiple_of((1 - par_ref[0]) * rows, 8)
    full_ref[pl.ds(at, rows), :] = mine_ref[...]
    full_ref[pl.ds(other, rows), :] = theirs_ref[...]


def lane_halves(par_ref, full_ref, keep_ref, send_ref):
    lanes = keep_ref.shape[1]
    at = pl.multiple_of(par_ref[0] * lanes, LANES)
    other = pl.multiple_of((1 - par_ref[0]) * lanes, LANES)
    keep_ref[...] = full_ref[:, pl.ds(at, lanes)]
    send_ref[...] = full_ref[:, pl.ds(other, lanes)]


def lane_joined(par_ref, mine_ref, theirs_ref, full_ref, start=0):
    lanes = mine_ref.shape[1]
    at = pl.multiple_of(start + par_ref[0] * lanes, LANES)
    other = pl.multiple_of(start + (1 - par_ref[0]) * lanes, LANES)
    full_ref[:, pl.ds(at, lanes)] = mine_ref[...]
    full_ref[:, pl.ds(other, lanes)] = theirs_ref[...]


def spans(block_refs):
    start, found = 0, []
    for ref in block_refs:
        found.append((start, ref))
        start += ref.shape[1]
    return found


def back_project(projected, block_refs, full_ref):
    parts = jnp.concatenate(thirds(projected), axis=0)
    for start, ref in spans(block_refs):
        tall = jnp.dot(parts, ref[...], preferred_element_type=F32)
        full_ref[:, start : start + ref.shape[1]] = fold(tall, projected.shape[0])


def forward_project(applied, block_refs):
    total = 0.0
    for start, ref in spans(block_refs):
        parts = jnp.concatenate(thirds(applied[:, start : start + ref.shape[1]]), axis=0)
        tall = lax.dot_general(parts, ref[...], (((1,), (1,)), ((), ())), preferred_element_type=F32)
        total = total + fold(tall, applied.shape[0])
    return total


def apply_first_body(masks, gathered, me_ref, par_ref, own_ref, twin_ref, *rest):
    pairs = rest[: len(masks)]
    rest = rest[len(masks) :]
    me = me_ref[0]
    days = own_ref.shape[1]
    if gathered:
        *pieces, block_ref, keep_ref, send_ref, proj_ref, full_ref = rest
        for mask, piece in enumerate(pieces):
            block_ref[pl.ds(pl.multiple_of((me ^ mask) * days, LANES), days), :] = piece[...]
    else:
        block_ref, keep_ref, send_ref, proj_ref, full_ref = rest

    def place(source, value):
        proj_ref[:, pl.ds(pl.multiple_of(source * days, LANES), days)] = value

    place(me, own_ref[...])
    place(me ^ 1, twin_ref[...])
    for mask, pair_ref in zip(masks, pairs):
        place(me ^ mask, pair_ref[0])
        place(me ^ mask ^ 1, pair_ref[1])
    back_project(proj_ref[...], [block_ref], full_ref)
    lane_halves(par_ref, full_ref, keep_ref, send_ref)


def apply_body(core_ref, par_ref, mine_ref, theirs_ref, *rest):
    *block_refs, keep_ref, send_ref, proj_ref, full_ref = rest
    joined(core_ref, mine_ref, theirs_ref, proj_ref)
    back_project(proj_ref[:, : block_refs[0].shape[0]], block_refs, full_ref)
    lane_halves(par_ref, full_ref, keep_ref, send_ref)


def gram_of(left, right):
    tall = lax.dot_general(
        jnp.concatenate(thirds(left), axis=0), jnp.concatenate(thirds(right), axis=0),
        (((1,), (1,)), ((), ())), preferred_element_type=F32,
    )
    rows, cols = left.shape[0], right.shape[0]
    part = [[tall[i * rows : (i + 1) * rows, k * cols : (k + 1) * cols] for k in range(3)] for i in range(3)]
    small = (part[0][2] + part[2][0]) + part[1][1]
    return ((part[2][2] + (part[1][2] + part[2][1])) + small) + (part[0][1] + part[1][0]) + part[0][0]


def widen(gram, lanes):
    return jnp.concatenate([gram, jnp.zeros((gram.shape[0], lanes - gram.shape[1]), F32)], axis=1)


def project_both_body(days_all, pieces, chunks, par_ref, core_ref, *rest):
    halves_refs = rest[: 2 * pieces]
    block_refs = rest[2 * pieces : 2 * pieces + chunks]
    *out_refs, full_ref, out_ref = rest[2 * pieces + chunks :]
    start = 0
    for k in range(pieces):
        mine_ref, theirs_ref = halves_refs[2 * k : 2 * k + 2]
        lane_joined(par_ref, mine_ref, theirs_ref, full_ref, start)
        start += 2 * mine_ref.shape[1]
    applied = full_ref[...] / days_all
    days = block_refs[0].shape[0]
    projected = forward_project(applied, block_refs)
    gram = gram_of(applied, applied)
    half = out_ref.shape[0]
    for k in range(2):
        out_ref[:, :days] = projected[k * half : (k + 1) * half]
        out_ref[:, days:] = widen(gram[k * half : (k + 1) * half], LANES)
        halves(core_ref, out_ref, *out_refs[2 * k : 2 * k + 2])


def project_lead_body(days_all, par_ref, core_ref, mine_ref, theirs_ref, *rest):
    *block_refs, inv_ref, keep_ref, send_ref, raw_ref, applied_ref, full_ref, out_ref = rest
    lane_joined(par_ref, mine_ref, theirs_ref, full_ref)
    raw = full_ref[...] / days_all
    half = full_ref.shape[0]
    applied = jnp.dot(inv_ref[:half, :half], raw, precision=HIGH, preferred_element_type=F32)
    raw_ref[...] = raw
    applied_ref[...] = applied
    days = block_refs[0].shape[0]
    out_ref[:, :days] = forward_project(applied, block_refs)
    out_ref[:, days:] = widen(gram_of(applied, applied), LANES)
    halves(core_ref, out_ref, keep_ref, send_ref)


def project_trail_body(days_all, par_ref, core_ref, mine_ref, theirs_ref, raw_ref, lead_ref, *rest):
    *block_refs, inv_ref, keep_ref, send_ref, full_ref, out_ref = rest
    lane_joined(par_ref, mine_ref, theirs_ref, full_ref)
    half = full_ref.shape[0]
    raw = jnp.concatenate([raw_ref[...], full_ref[...] / days_all], axis=0)
    applied = jnp.dot(inv_ref[half:, :], raw, precision=HIGH, preferred_element_type=F32)
    days = block_refs[0].shape[0]
    out_ref[:, :days] = forward_project(applied, block_refs)
    both = jnp.concatenate([lead_ref[...], applied], axis=0)
    out_ref[:, days:] = widen(gram_of(applied, both), LANES)
    halves(core_ref, out_ref, keep_ref, send_ref)


def eliminate(gram):
    size = gram.shape[0]
    rows = lax.broadcasted_iota(jnp.int32, (size, 2 * size), 0)
    lanes = lax.broadcasted_iota(jnp.int32, (size, 2 * size), 1)
    work = jnp.concatenate([gram, jnp.zeros_like(gram)], axis=1)
    work = jnp.where(lanes == rows + size, 1.0, work)
    for first in range(0, size, GROUP):
        columns = [jnp.broadcast_to(work[:, first + j : first + j + 1], work.shape) for j in range(GROUP)]
        for j in range(GROUP):
            k = first + j
            inverse = 1.0 / columns[j][k : k + 1, :]
            below = jnp.where(rows > k, columns[j], 0.0)
            for later in range(j + 1, GROUP):
                columns[later] = columns[later] - below * (columns[later][k : k + 1, :] * inverse)
            work = work - below * (work[k : k + 1, :] * inverse)
    on_diag = jnp.where(lanes == rows, work, 0.0)
    pivots = jnp.sqrt(jnp.sum(on_diag, axis=1, keepdims=True))
    diag_row = jnp.sqrt(jnp.sum(on_diag, axis=0, keepdims=True))[:, :size]
    return work[:, size:] / pivots, diag_row


def factor_body(days, core_ref, mine_ref, theirs_ref, mine_late_ref, theirs_late_ref, inv_ref, diag_ref, full_ref):
    joined(core_ref, mine_ref, theirs_ref, full_ref)
    size = inv_ref.shape[0]
    half = size // 2
    lead = full_ref[:, days : days + half]
    joined(core_ref, mine_late_ref, theirs_late_ref, full_ref)
    trail = full_ref[:, days : days + size]
    top = jnp.concatenate([lead, trail[:, :half].T], axis=1)
    inverse, diag_row = eliminate(jnp.concatenate([top, trail], axis=0))
    inv_ref[...] = inverse
    diag_ref[...] = diag_row


def last_gram_body(days_all, lead_ref, trail_ref, inv_ref, applied_ref, gram_ref):
    raw = jnp.concatenate([lead_ref[...], trail_ref[...]], axis=0) / days_all
    applied = jnp.dot(inv_ref[...], raw, precision=HIGH, preferred_element_type=F32)
    applied_ref[...] = applied
    gram = gram_of(applied, applied)
    half = gram_ref.shape[0]
    gram_ref[...] = jnp.concatenate([gram[:half], gram[half:]], axis=1)


def last_body(scale, par_ref, mine_ref, theirs_ref, gram_ref, *rest):
    diag_refs = rest[: ITERS - 1]
    out_ref, strengths_ref, full_ref = rest[ITERS - 1 :]
    lane_joined(par_ref, mine_ref, theirs_ref, full_ref)
    factors = full_ref.shape[0]
    gram = jnp.concatenate([gram_ref[:, :factors], gram_ref[:, factors:]], axis=0)
    inverse, diag_row = eliminate(gram)
    out_ref[...] = jnp.dot(inverse, full_ref[...], precision=HIGH, preferred_element_type=F32) * scale
    for k, ref in enumerate(diag_refs):
        strengths_ref[k : k + 1, :] = ref[...]
    strengths_ref[ITERS - 1 : ITERS, :] = diag_row


def swap(x, axis, mask):
    size = lax.axis_size(axis)
    return lax.ppermute(x, axis, [(s, s ^ mask) for s in range(size)])


def cross(x, gr_mask, gc_mask):
    gr, gc = lax.axis_size("gr"), lax.axis_size("gc")
    pairs = [(g * gc + c, (g ^ gr_mask) * gc + (c ^ gc_mask)) for g in range(gr) for c in range(gc)]
    return lax.ppermute(x, ("gr", "gc"), pairs)


def tree(parts):
    while len(parts) > 1:
        parts = [parts[i] + parts[i + 1] for i in range(0, len(parts), 2)]
    return parts[0]


def sum_chips(x):
    size = lax.axis_size("gr")
    return tree([x if m == 0 else swap(x, "gr", m) for m in range(0, size, 2)])


def sum_days(keep, send):
    size = lax.axis_size("gc")
    mine = keep + swap(send, "gc", 1)
    mask = 2
    while mask < size:
        mine = mine + swap(mine, "gc", mask)
        mask *= 2
    return mine


def sum_assets(keep, send):
    mine = sum_chips(keep + swap(send, "gr", 1))
    return mine, swap(mine, "gr", 1)


def local(returns, start_seed):
    days, assets = returns.shape
    factors = start_seed.shape[1]
    blocks, slabs = lax.axis_size("gr"), lax.axis_size("gc")
    span = assets // blocks
    slab_days = days * blocks
    days_all = slab_days * slabs
    core = (lax.axis_index("gr") % 2).astype(jnp.int32).reshape(1)
    par = (lax.axis_index("gc") % 2).astype(jnp.int32).reshape(1)
    me = lax.axis_index("gr").astype(jnp.int32).reshape(1)
    half = factors // 2
    packed_width = slab_days + LANES
    dots = 6 * factors * slab_days * span

    unit = 2 * LANES
    cut = span * CUT // 8 // unit * unit
    rest = span - cut
    masks = tuple(range(2, blocks, 2))

    dealt = deal(returns, blocks, cut)
    block = lax.all_to_all(dealt, "gr", 0, 0).reshape(slab_days, cut)
    own, *pieces = call(
        functools.partial(project_first_body, span),
        [((factors, days), F32)] + [((days, rest), BF16)] * blocks,
        [me], [returns, start_seed.T], 4 * days * assets * factors,
    )
    twin = swap(own, "gr", 1)
    both = jnp.stack([own, twin])
    pairs = [swap(both, "gr", m) for m in masks]
    pieces = [p if m == 0 else swap(p, "gr", m) for m, p in enumerate(pieces)]

    asset_half = ((factors, span // 2), F32)
    full_assets = pltpu.VMEM((factors, span), F32)
    slab = pltpu.VMEM((factors, slab_days), F32)

    shared = [own, twin, *pairs]
    keep, send = call(
        functools.partial(apply_first_body, masks, False), [((factors, cut // 2), F32)] * 2, [me, par],
        shared + [block], dots, [slab, pltpu.VMEM((factors, cut), F32)],
    )
    mine = sum_days(keep, send)
    theirs = swap(mine, "gc", 1)
    last, keep, send = call(
        functools.partial(apply_first_body, masks, True),
        [((slab_days, rest), BF16)] + [((factors, rest // 2), F32)] * 2, [me, par],
        shared + pieces, dots, [slab, pltpu.VMEM((factors, rest), F32)],
    )
    mine_late = sum_days(keep, send)
    pieces = [mine, theirs, mine_late, swap(mine_late, "gc", 1)]
    block_list = [block, last]
    quarter = ((half // 2, packed_width), F32)
    rows = ((half, span), F32)
    part_assets = pltpu.VMEM((half, span), F32)
    part_days = pltpu.VMEM((half, packed_width), F32)
    lane_half = ((half, span // 2), F32)
    diagonals = []
    for sweep in range(ITERS - 1):
        if sweep:
            mine = sum_days(*sent[0])
            keep, send, raw, applied = call(
                functools.partial(project_lead_body, days_all), [quarter] * 2 + [rows] * 2, [par, core],
                [mine, swap(mine, "gc", 1), *block_list, inverse], dots // 2, [part_assets, part_days],
            )
            lead = sum_assets(keep, send)
            mine = sum_days(*sent[1])
            keep, send = call(
                functools.partial(project_trail_body, days_all), [quarter] * 2, [par, core],
                [mine, swap(mine, "gc", 1), raw, applied, *block_list, inverse], dots // 2,
                [part_assets, part_days],
            )
            trail = sum_assets(keep, send)
        else:
            parts = call(
                functools.partial(project_both_body, days_all, len(pieces) // 2, len(block_list)),
                [quarter] * 4, [par, core], pieces + block_list, dots, [full_assets, part_days],
            )
            lead = sum_assets(*parts[:2])
            trail = sum_assets(*parts[2:])
        sent = [
            call(apply_body, [lane_half] * 2, [core, par], [*pair, *block_list], dots // 2, [part_days, part_assets])
            for pair in (lead, trail)
        ]
        inverse, diag_row = call(
            functools.partial(factor_body, slab_days),
            [((factors, factors), F32), ((1, factors), F32)], [core], [*lead, *trail], dots // 2, [part_days],
        )
        diagonals.append(diag_row)
    lead = sum_days(*sent[0])
    trail = sum_days(*sent[1])
    applied, gram = call(
        functools.partial(last_gram_body, days_all),
        [asset_half, ((half, 2 * factors), F32)], [], [lead, trail, inverse], dots,
    )
    theirs = swap(applied, "gc", 1)
    gram = (gram + cross(gram, 1, 0)) + (cross(gram, 0, 1) + cross(gram, 1, 1))
    gram = sum_chips(gram)
    loadings, strengths = call(
        functools.partial(last_body, math.sqrt(assets)),
        [((factors, span), F32), ((ITERS, factors), F32)], [par],
        [applied, theirs, gram, *diagonals], dots, [full_assets],
    )
    return loadings.T, strengths


def solution(mesh):
    placed = (P(("gr", "gc"), None), P())
    return jax.shard_map(local, mesh=mesh, in_specs=placed, out_specs=(P("gr", None), P()), check_vma=False)
```

```python
import functools
import math

import jax
import jax.numpy as jnp
from jax import lax
from jax.experimental import pallas as pl
from jax.experimental.pallas import tpu as pltpu
from jax.sharding import PartitionSpec as P

ITERS = 3
LANES = 128
GROUP = 16
CUT = 4
HIGH = lax.Precision.HIGHEST
F32 = jnp.float32
BF16 = jnp.bfloat16


def vmem(count):
    return [pl.BlockSpec(memory_space=pltpu.VMEM)] * count


def smem():
    return [pl.BlockSpec(memory_space=pltpu.SMEM)]


def call(body, outs, scalars, arrays, flops, scratch=()):
    in_specs = smem() * len(scalars) + vmem(len(arrays))
    moved = sum(math.prod(o[0]) * 4 for o in outs)
    return pl.pallas_call(
        body,
        out_shape=[jax.ShapeDtypeStruct(shape, dtype) for shape, dtype in outs],
        in_specs=in_specs,
        out_specs=vmem(len(outs)),
        scratch_shapes=list(scratch),
        cost_estimate=pl.CostEstimate(flops=flops, bytes_accessed=moved, transcendentals=0),
        compiler_params=pltpu.CompilerParams(vmem_limit_bytes=16 * 1024 * 1024),
    )(*scalars, *arrays)


def thirds(x):
    top = x.astype(BF16)
    rest = x - top.astype(F32)
    mid = rest.astype(BF16)
    low = (rest - mid.astype(F32)).astype(BF16)
    return top, mid, low


def fold(tall, rows):
    return tall[2 * rows :] + tall[rows : 2 * rows] + tall[:rows]


def open_body(me_ref, returns_ref, seed_ref, out_ref, *rest):
    *pieces, dealt_ref, wide_ref, table_ref, sems = rest
    blocks, _, width = dealt_ref.shape
    span = returns_ref.shape[1] // blocks
    copies = [
        pltpu.make_async_copy(returns_ref, wide_ref, sems.at[0]),
        pltpu.make_async_copy(seed_ref, table_ref, sems.at[1]),
    ]
    for mask, piece in enumerate(pieces):
        at = pl.multiple_of((me_ref[0] ^ mask) * span, LANES)
        source = returns_ref.at[:, pl.ds(at, piece.shape[1])]
        copies.append(pltpu.make_async_copy(source, piece, sems.at[2 + mask]))
    for copy in copies:
        copy.start()
    for copy in copies[:2]:
        copy.wait()
    factors = out_ref.shape[0]
    seed = table_ref[...]
    coarse = (seed >> 3) << 3
    fine = seed - coarse
    both = jnp.concatenate([coarse.astype(F32).astype(BF16), fine.astype(F32).astype(BF16)], axis=0)
    tall = lax.dot_general(both, wide_ref[...], (((1,), (1,)), ((), ())), preferred_element_type=F32)
    out_ref[...] = (tall[:factors] + tall[factors:]) / 1000.0
    for b in range(blocks):
        dealt_ref[b] = wide_ref[:, (b + 1) * span - width : (b + 1) * span]
    for copy in copies[2:]:
        copy.wait()


def opening(me, returns, seed, blocks, width):
    days, assets = returns.shape
    rest = assets // blocks - width
    factors = seed.shape[0]
    outs = [((factors, days), F32)] + [((days, width), BF16)] * blocks + [((blocks, days, rest), BF16)]
    return pl.pallas_call(
        open_body,
        out_shape=[jax.ShapeDtypeStruct(shape, dtype) for shape, dtype in outs],
        in_specs=smem() + [pl.BlockSpec(memory_space=pltpu.HBM)] * 2,
        out_specs=vmem(len(outs)),
        scratch_shapes=[
            pltpu.VMEM(returns.shape, BF16),
            pltpu.VMEM(seed.shape, jnp.int32),
            pltpu.SemaphoreType.DMA((2 + blocks,)),
        ],
        cost_estimate=pl.CostEstimate(
            flops=4 * days * assets * factors, bytes_accessed=returns.size * 2, transcendentals=0
        ),
        compiler_params=pltpu.CompilerParams(vmem_limit_bytes=51 * 1024 * 1024),
    )(me, returns, seed)


def halves(par_ref, full_ref, keep_ref, send_ref):
    rows = keep_ref.shape[0]
    at = pl.multiple_of(par_ref[0] * rows, 8)
    other = pl.multiple_of((1 - par_ref[0]) * rows, 8)
    keep_ref[...] = full_ref[pl.ds(at, rows), :]
    send_ref[...] = full_ref[pl.ds(other, rows), :]


def joined(par_ref, mine_ref, theirs_ref, full_ref):
    rows = mine_ref.shape[0]
    at = pl.multiple_of(par_ref[0] * rows, 8)
    other = pl.multiple_of((1 - par_ref[0]) * rows, 8)
    full_ref[pl.ds(at, rows), :] = mine_ref[...]
    full_ref[pl.ds(other, rows), :] = theirs_ref[...]


def lane_halves(par_ref, full_ref, keep_ref, send_ref):
    lanes = keep_ref.shape[1]
    at = pl.multiple_of(par_ref[0] * lanes, LANES)
    other = pl.multiple_of((1 - par_ref[0]) * lanes, LANES)
    keep_ref[...] = full_ref[:, pl.ds(at, lanes)]
    send_ref[...] = full_ref[:, pl.ds(other, lanes)]


def lane_joined(par_ref, mine_ref, theirs_ref, full_ref, start=0):
    lanes = mine_ref.shape[1]
    at = pl.multiple_of(start + par_ref[0] * lanes, LANES)
    other = pl.multiple_of(start + (1 - par_ref[0]) * lanes, LANES)
    full_ref[:, pl.ds(at, lanes)] = mine_ref[...]
    full_ref[:, pl.ds(other, lanes)] = theirs_ref[...]


def spans(block_refs):
    start, found = 0, []
    for ref in block_refs:
        found.append((start, ref))
        start += ref.shape[1]
    return found


def back_project(projected, block_refs, full_ref):
    parts = jnp.concatenate(thirds(projected), axis=0)
    for start, ref in spans(block_refs):
        tall = jnp.dot(parts, ref[...], preferred_element_type=F32)
        full_ref[:, start : start + ref.shape[1]] = fold(tall, projected.shape[0])


def forward_project(applied, block_refs):
    total = 0.0
    for start, ref in spans(block_refs):
        parts = jnp.concatenate(thirds(applied[:, start : start + ref.shape[1]]), axis=0)
        tall = lax.dot_general(parts, ref[...], (((1,), (1,)), ((), ())), preferred_element_type=F32)
        total = total + fold(tall, applied.shape[0])
    return total


def apply_first_body(masks, gathered, me_ref, par_ref, own_ref, twin_ref, *rest):
    pairs = rest[: len(masks)]
    rest = rest[len(masks) :]
    me = me_ref[0]
    days = own_ref.shape[1]
    if gathered:
        *pieces, block_ref, keep_ref, send_ref, proj_ref, full_ref = rest
        for mask, piece in enumerate(pieces):
            block_ref[pl.ds(pl.multiple_of((me ^ mask) * days, LANES), days), :] = piece[...]
    else:
        block_ref, keep_ref, send_ref, proj_ref, full_ref = rest

    def place(source, value):
        proj_ref[:, pl.ds(pl.multiple_of(source * days, LANES), days)] = value

    place(me, own_ref[...])
    place(me ^ 1, twin_ref[...])
    for mask, pair_ref in zip(masks, pairs):
        place(me ^ mask, pair_ref[0])
        place(me ^ mask ^ 1, pair_ref[1])
    back_project(proj_ref[...], [block_ref], full_ref)
    lane_halves(par_ref, full_ref, keep_ref, send_ref)


def apply_body(core_ref, par_ref, mine_ref, theirs_ref, *rest):
    *block_refs, keep_ref, send_ref, proj_ref, full_ref = rest
    joined(core_ref, mine_ref, theirs_ref, proj_ref)
    back_project(proj_ref[:, : block_refs[0].shape[0]], block_refs, full_ref)
    lane_halves(par_ref, full_ref, keep_ref, send_ref)


def gram_of(left, right):
    tall = lax.dot_general(
        jnp.concatenate(thirds(left), axis=0), jnp.concatenate(thirds(right), axis=0),
        (((1,), (1,)), ((), ())), preferred_element_type=F32,
    )
    rows, cols = left.shape[0], right.shape[0]
    part = [[tall[i * rows : (i + 1) * rows, k * cols : (k + 1) * cols] for k in range(3)] for i in range(3)]
    small = (part[0][2] + part[2][0]) + part[1][1]
    return ((part[2][2] + (part[1][2] + part[2][1])) + small) + (part[0][1] + part[1][0]) + part[0][0]


def widen(gram, lanes):
    return jnp.concatenate([gram, jnp.zeros((gram.shape[0], lanes - gram.shape[1]), F32)], axis=1)


def project_both_body(days_all, pieces, chunks, par_ref, core_ref, *rest):
    halves_refs = rest[: 2 * pieces]
    block_refs = rest[2 * pieces : 2 * pieces + chunks]
    *out_refs, full_ref, out_ref = rest[2 * pieces + chunks :]
    start = 0
    for k in range(pieces):
        mine_ref, theirs_ref = halves_refs[2 * k : 2 * k + 2]
        lane_joined(par_ref, mine_ref, theirs_ref, full_ref, start)
        start += 2 * mine_ref.shape[1]
    applied = full_ref[...] / days_all
    days = block_refs[0].shape[0]
    projected = forward_project(applied, block_refs)
    gram = gram_of(applied, applied)
    half = out_ref.shape[0]
    for k in range(2):
        out_ref[:, :days] = projected[k * half : (k + 1) * half]
        out_ref[:, days:] = widen(gram[k * half : (k + 1) * half], LANES)
        halves(core_ref, out_ref, *out_refs[2 * k : 2 * k + 2])


def project_lead_body(days_all, par_ref, core_ref, mine_ref, theirs_ref, *rest):
    *block_refs, inv_ref, keep_ref, send_ref, raw_ref, applied_ref, full_ref, out_ref = rest
    lane_joined(par_ref, mine_ref, theirs_ref, full_ref)
    raw = full_ref[...] / days_all
    half = full_ref.shape[0]
    applied = jnp.dot(inv_ref[:half, :half], raw, precision=HIGH, preferred_element_type=F32)
    raw_ref[...] = raw
    applied_ref[...] = applied
    days = block_refs[0].shape[0]
    out_ref[:, :days] = forward_project(applied, block_refs)
    out_ref[:, days:] = widen(gram_of(applied, applied), LANES)
    halves(core_ref, out_ref, keep_ref, send_ref)


def project_trail_body(days_all, par_ref, core_ref, mine_ref, theirs_ref, raw_ref, lead_ref, *rest):
    *block_refs, inv_ref, keep_ref, send_ref, full_ref, out_ref = rest
    lane_joined(par_ref, mine_ref, theirs_ref, full_ref)
    half = full_ref.shape[0]
    raw = jnp.concatenate([raw_ref[...], full_ref[...] / days_all], axis=0)
    applied = jnp.dot(inv_ref[half:, :], raw, precision=HIGH, preferred_element_type=F32)
    days = block_refs[0].shape[0]
    out_ref[:, :days] = forward_project(applied, block_refs)
    both = jnp.concatenate([lead_ref[...], applied], axis=0)
    out_ref[:, days:] = widen(gram_of(applied, both), LANES)
    halves(core_ref, out_ref, keep_ref, send_ref)


def eliminate(gram):
    size = gram.shape[0]
    rows = lax.broadcasted_iota(jnp.int32, (size, 2 * size), 0)
    lanes = lax.broadcasted_iota(jnp.int32, (size, 2 * size), 1)
    work = jnp.concatenate([gram, jnp.zeros_like(gram)], axis=1)
    work = jnp.where(lanes == rows + size, 1.0, work)
    for first in range(0, size, GROUP):
        columns = [jnp.broadcast_to(work[:, first + j : first + j + 1], work.shape) for j in range(GROUP)]
        for j in range(GROUP):
            k = first + j
            inverse = 1.0 / columns[j][k : k + 1, :]
            below = jnp.where(rows > k, columns[j], 0.0)
            for later in range(j + 1, GROUP):
                columns[later] = columns[later] - below * (columns[later][k : k + 1, :] * inverse)
            work = work - below * (work[k : k + 1, :] * inverse)
    on_diag = jnp.where(lanes == rows, work, 0.0)
    pivots = jnp.sqrt(jnp.sum(on_diag, axis=1, keepdims=True))
    diag_row = jnp.sqrt(jnp.sum(on_diag, axis=0, keepdims=True))[:, :size]
    return work[:, size:] / pivots, diag_row


def factor_body(days, core_ref, mine_ref, theirs_ref, mine_late_ref, theirs_late_ref, inv_ref, diag_ref, full_ref):
    joined(core_ref, mine_ref, theirs_ref, full_ref)
    size = inv_ref.shape[0]
    half = size // 2
    lead = full_ref[:, days : days + half]
    joined(core_ref, mine_late_ref, theirs_late_ref, full_ref)
    trail = full_ref[:, days : days + size]
    top = jnp.concatenate([lead, trail[:, :half].T], axis=1)
    inverse, diag_row = eliminate(jnp.concatenate([top, trail], axis=0))
    inv_ref[...] = inverse
    diag_ref[...] = diag_row


def last_gram_body(days_all, lead_ref, trail_ref, inv_ref, applied_ref, gram_ref):
    raw = jnp.concatenate([lead_ref[...], trail_ref[...]], axis=0) / days_all
    applied = jnp.dot(inv_ref[...], raw, precision=HIGH, preferred_element_type=F32)
    applied_ref[...] = applied
    gram = gram_of(applied, applied)
    half = gram_ref.shape[0]
    gram_ref[...] = jnp.concatenate([gram[:half], gram[half:]], axis=1)


def last_body(scale, par_ref, mine_ref, theirs_ref, gram_ref, *rest):
    diag_refs = rest[: ITERS - 1]
    out_ref, strengths_ref, full_ref = rest[ITERS - 1 :]
    lane_joined(par_ref, mine_ref, theirs_ref, full_ref)
    factors = full_ref.shape[0]
    gram = jnp.concatenate([gram_ref[:, :factors], gram_ref[:, factors:]], axis=0)
    inverse, diag_row = eliminate(gram)
    out_ref[...] = jnp.dot(inverse, full_ref[...], precision=HIGH, preferred_element_type=F32) * scale
    for k, ref in enumerate(diag_refs):
        strengths_ref[k : k + 1, :] = ref[...]
    strengths_ref[ITERS - 1 : ITERS, :] = diag_row


def swap(x, axis, mask):
    size = lax.axis_size(axis)
    return lax.ppermute(x, axis, [(s, s ^ mask) for s in range(size)])


def cross(x, gr_mask, gc_mask):
    gr, gc = lax.axis_size("gr"), lax.axis_size("gc")
    pairs = [(g * gc + c, (g ^ gr_mask) * gc + (c ^ gc_mask)) for g in range(gr) for c in range(gc)]
    return lax.ppermute(x, ("gr", "gc"), pairs)


def tree(parts):
    while len(parts) > 1:
        parts = [parts[i] + parts[i + 1] for i in range(0, len(parts), 2)]
    return parts[0]


def sum_chips(x):
    size = lax.axis_size("gr")
    return tree([x if m == 0 else swap(x, "gr", m) for m in range(0, size, 2)])


def sum_days(keep, send):
    size = lax.axis_size("gc")
    mine = keep + swap(send, "gc", 1)
    mask = 2
    while mask < size:
        mine = mine + swap(mine, "gc", mask)
        mask *= 2
    return mine


def sum_assets(keep, send, reverse):
    mine = keep + swap(send, "gr", 1)
    size = lax.axis_size("gr")
    masks = [m for m in (1 << k for k in range(1, size)) if m < size]
    for mask in masks[::-1] if reverse else masks:
        mine = mine + swap(mine, "gr", mask)
    return mine, swap(mine, "gr", 1)


def local(returns, start_seed):
    days, assets = returns.shape
    factors = start_seed.shape[1]
    blocks, slabs = lax.axis_size("gr"), lax.axis_size("gc")
    span = assets // blocks
    slab_days = days * blocks
    days_all = slab_days * slabs
    core = (lax.axis_index("gr") % 2).astype(jnp.int32).reshape(1)
    par = (lax.axis_index("gc") % 2).astype(jnp.int32).reshape(1)
    me = lax.axis_index("gr").astype(jnp.int32).reshape(1)
    half = factors // 2
    packed_width = slab_days + LANES
    dots = 6 * factors * slab_days * span

    unit = 2 * LANES
    cut = span * CUT // 8 // unit * unit
    rest = span - cut
    masks = tuple(range(2, blocks, 2))

    own, *pieces, dealt = opening(me, returns, start_seed.T, blocks, cut)
    twin = swap(own, "gr", 1)
    both = jnp.stack([own, twin])
    pairs = [swap(both, "gr", m) for m in masks]
    pieces = [p if m == 0 else swap(p, "gr", m) for m, p in enumerate(pieces)]
    last = lax.all_to_all(dealt, "gr", 0, 0).reshape(slab_days, rest)

    asset_half = ((factors, span // 2), F32)
    full_assets = pltpu.VMEM((factors, span), F32)
    slab = pltpu.VMEM((factors, slab_days), F32)

    shared = [own, twin, *pairs]
    block, keep, send = call(
        functools.partial(apply_first_body, masks, True),
        [((slab_days, cut), BF16)] + [((factors, cut // 2), F32)] * 2, [me, par],
        shared + pieces, dots, [slab, pltpu.VMEM((factors, cut), F32)],
    )
    mine = sum_days(keep, send)
    theirs = swap(mine, "gc", 1)
    keep, send = call(
        functools.partial(apply_first_body, masks, False), [((factors, rest // 2), F32)] * 2, [me, par],
        shared + [last], dots, [slab, pltpu.VMEM((factors, rest), F32)],
    )
    mine_late = sum_days(keep, send)
    pieces = [mine, theirs, mine_late, swap(mine_late, "gc", 1)]
    block_list = [block, last]
    quarter = ((half // 2, packed_width), F32)
    rows = ((half, span), F32)
    part_assets = pltpu.VMEM((half, span), F32)
    part_days = pltpu.VMEM((half, packed_width), F32)
    lane_half = ((half, span // 2), F32)
    diagonals = []
    for sweep in range(ITERS - 1):
        if sweep:
            mine = sum_days(*sent[0])
            keep, send, raw, applied = call(
                functools.partial(project_lead_body, days_all), [quarter] * 2 + [rows] * 2, [par, core],
                [mine, swap(mine, "gc", 1), *block_list, inverse], dots // 2, [part_assets, part_days],
            )
            lead = sum_assets(keep, send, False)
            mine = sum_days(*sent[1])
            keep, send = call(
                functools.partial(project_trail_body, days_all), [quarter] * 2, [par, core],
                [mine, swap(mine, "gc", 1), raw, applied, *block_list, inverse], dots // 2,
                [part_assets, part_days],
            )
            trail = sum_assets(keep, send, True)
        else:
            parts = call(
                functools.partial(project_both_body, days_all, len(pieces) // 2, len(block_list)),
                [quarter] * 4, [par, core], pieces + block_list, dots, [full_assets, part_days],
            )
            lead = sum_assets(*parts[:2], False)
            trail = sum_assets(*parts[2:], True)
        sent = [
            call(apply_body, [lane_half] * 2, [core, par], [*pair, *block_list], dots // 2, [part_days, part_assets])
            for pair in (lead, trail)
        ]
        inverse, diag_row = call(
            functools.partial(factor_body, slab_days),
            [((factors, factors), F32), ((1, factors), F32)], [core], [*lead, *trail], dots // 2, [part_days],
        )
        diagonals.append(diag_row)
    lead = sum_days(*sent[0])
    trail = sum_days(*sent[1])
    applied, gram = call(
        functools.partial(last_gram_body, days_all),
        [asset_half, ((half, 2 * factors), F32)], [], [lead, trail, inverse], dots,
    )
    theirs = swap(applied, "gc", 1)
    gram = (gram + cross(gram, 1, 0)) + (cross(gram, 0, 1) + cross(gram, 1, 1))
    gram = sum_chips(gram)
    loadings, strengths = call(
        functools.partial(last_body, math.sqrt(assets)),
        [((factors, span), F32), ((ITERS, factors), F32)], [par],
        [applied, theirs, gram, *diagonals], dots, [full_assets],
    )
    return loadings.T, strengths


def solution(mesh):
    placed = (P(("gr", "gc"), None), P())
    return jax.shard_map(local, mesh=mesh, in_specs=placed, out_specs=(P("gr", None), P()), check_vma=False)
```

```python
import functools
import math

import jax
import jax.numpy as jnp
from jax import lax
from jax.experimental import pallas as pl
from jax.experimental.pallas import tpu as pltpu
from jax.sharding import PartitionSpec as P

ITERS = 3
LANES = 128
GROUP = 16
CUT = 4
HIGH = lax.Precision.HIGHEST
F32 = jnp.float32
BF16 = jnp.bfloat16


def vmem(count):
    return [pl.BlockSpec(memory_space=pltpu.VMEM)] * count


def smem():
    return [pl.BlockSpec(memory_space=pltpu.SMEM)]


def call(body, outs, scalars, arrays, flops, scratch=()):
    in_specs = smem() * len(scalars) + vmem(len(arrays))
    moved = sum(math.prod(o[0]) * 4 for o in outs)
    return pl.pallas_call(
        body,
        out_shape=[jax.ShapeDtypeStruct(shape, dtype) for shape, dtype in outs],
        in_specs=in_specs,
        out_specs=vmem(len(outs)),
        scratch_shapes=list(scratch),
        cost_estimate=pl.CostEstimate(flops=flops, bytes_accessed=moved, transcendentals=0),
        compiler_params=pltpu.CompilerParams(vmem_limit_bytes=16 * 1024 * 1024),
    )(*scalars, *arrays)


def thirds(x):
    top = x.astype(BF16)
    rest = x - top.astype(F32)
    mid = rest.astype(BF16)
    low = (rest - mid.astype(F32)).astype(BF16)
    return top, mid, low


def fold(tall, rows):
    return tall[2 * rows :] + tall[rows : 2 * rows] + tall[:rows]


def open_body(me_ref, returns_ref, seed_ref, out_ref, *rest):
    *pieces, dealt_ref, wide_ref, table_ref, sems = rest
    blocks, _, width = dealt_ref.shape
    span = returns_ref.shape[1] // blocks
    copies = [
        pltpu.make_async_copy(returns_ref, wide_ref, sems.at[0]),
        pltpu.make_async_copy(seed_ref, table_ref, sems.at[1]),
    ]
    for mask, piece in enumerate(pieces):
        at = pl.multiple_of((me_ref[0] ^ mask) * span, LANES)
        source = returns_ref.at[:, pl.ds(at, piece.shape[1])]
        copies.append(pltpu.make_async_copy(source, piece, sems.at[2 + mask]))
    for copy in copies:
        copy.start()
    copies[0].wait()
    deals = [
        pltpu.make_async_copy(
            wide_ref.at[:, (b + 1) * span - width : (b + 1) * span], dealt_ref.at[b], sems.at[2 + blocks + b]
        )
        for b in range(blocks)
    ]
    for deal in deals:
        deal.start()
    copies[1].wait()
    factors = out_ref.shape[0]
    seed = table_ref[...]
    coarse = (seed >> 3) << 3
    fine = seed - coarse
    both = jnp.concatenate([coarse.astype(F32).astype(BF16), fine.astype(F32).astype(BF16)], axis=0)
    tall = lax.dot_general(both, wide_ref[...], (((1,), (1,)), ((), ())), preferred_element_type=F32)
    out_ref[...] = (tall[:factors] + tall[factors:]) / 1000.0
    for copy in copies[2:] + deals:
        copy.wait()


def opening(me, returns, seed, blocks, width):
    days, assets = returns.shape
    rest = assets // blocks - width
    factors = seed.shape[0]
    outs = [((factors, days), F32)] + [((days, width), BF16)] * blocks + [((blocks, days, rest), BF16)]
    return pl.pallas_call(
        open_body,
        out_shape=[jax.ShapeDtypeStruct(shape, dtype) for shape, dtype in outs],
        in_specs=smem() + [pl.BlockSpec(memory_space=pltpu.HBM)] * 2,
        out_specs=vmem(len(outs) - 1) + [pl.BlockSpec(memory_space=pltpu.HBM)],
        scratch_shapes=[
            pltpu.VMEM(returns.shape, BF16),
            pltpu.VMEM(seed.shape, jnp.int32),
            pltpu.SemaphoreType.DMA((2 + 2 * blocks,)),
        ],
        cost_estimate=pl.CostEstimate(
            flops=4 * days * assets * factors, bytes_accessed=returns.size * 2, transcendentals=0
        ),
        compiler_params=pltpu.CompilerParams(vmem_limit_bytes=51 * 1024 * 1024),
    )(me, returns, seed)


def halves(par_ref, full_ref, keep_ref, send_ref):
    rows = keep_ref.shape[0]
    at = pl.multiple_of(par_ref[0] * rows, 8)
    other = pl.multiple_of((1 - par_ref[0]) * rows, 8)
    keep_ref[...] = full_ref[pl.ds(at, rows), :]
    send_ref[...] = full_ref[pl.ds(other, rows), :]


def joined(par_ref, mine_ref, theirs_ref, full_ref):
    rows = mine_ref.shape[0]
    at = pl.multiple_of(par_ref[0] * rows, 8)
    other = pl.multiple_of((1 - par_ref[0]) * rows, 8)
    full_ref[pl.ds(at, rows), :] = mine_ref[...]
    full_ref[pl.ds(other, rows), :] = theirs_ref[...]


def lane_halves(par_ref, full_ref, keep_ref, send_ref):
    lanes = keep_ref.shape[1]
    at = pl.multiple_of(par_ref[0] * lanes, LANES)
    other = pl.multiple_of((1 - par_ref[0]) * lanes, LANES)
    keep_ref[...] = full_ref[:, pl.ds(at, lanes)]
    send_ref[...] = full_ref[:, pl.ds(other, lanes)]


def lane_joined(par_ref, mine_ref, theirs_ref, full_ref, start=0):
    lanes = mine_ref.shape[1]
    at = pl.multiple_of(start + par_ref[0] * lanes, LANES)
    other = pl.multiple_of(start + (1 - par_ref[0]) * lanes, LANES)
    full_ref[:, pl.ds(at, lanes)] = mine_ref[...]
    full_ref[:, pl.ds(other, lanes)] = theirs_ref[...]


def spans(block_refs):
    start, found = 0, []
    for ref in block_refs:
        found.append((start, ref))
        start += ref.shape[1]
    return found


def back_project(projected, block_refs, full_ref):
    parts = jnp.concatenate(thirds(projected), axis=0)
    for start, ref in spans(block_refs):
        tall = jnp.dot(parts, ref[...], preferred_element_type=F32)
        full_ref[:, start : start + ref.shape[1]] = fold(tall, projected.shape[0])


def forward_project(applied, block_refs):
    total = 0.0
    for start, ref in spans(block_refs):
        parts = jnp.concatenate(thirds(applied[:, start : start + ref.shape[1]]), axis=0)
        tall = lax.dot_general(parts, ref[...], (((1,), (1,)), ((), ())), preferred_element_type=F32)
        total = total + fold(tall, applied.shape[0])
    return total


def apply_first_body(count, gathered, me_ref, par_ref, *rest):
    slabs, rest = rest[:count], rest[count:]
    me = me_ref[0]
    days = slabs[0].shape[1]

    def source(mask):
        return pl.ds(pl.multiple_of((me ^ mask) * days, LANES), days)

    if gathered:
        *pieces, block_ref, keep_ref, send_ref, proj_ref, full_ref = rest
        for mask, piece in enumerate(pieces):
            block_ref[source(mask), :] = piece[...]
    else:
        block_ref, keep_ref, send_ref, proj_ref, full_ref = rest
    for mask, ref in enumerate(slabs):
        proj_ref[:, source(mask)] = ref[...]
    back_project(proj_ref[...], [block_ref], full_ref)
    lane_halves(par_ref, full_ref, keep_ref, send_ref)


def apply_body(core_ref, par_ref, mine_ref, theirs_ref, *rest):
    *block_refs, keep_ref, send_ref, proj_ref, full_ref = rest
    joined(core_ref, mine_ref, theirs_ref, proj_ref)
    back_project(proj_ref[:, : block_refs[0].shape[0]], block_refs, full_ref)
    lane_halves(par_ref, full_ref, keep_ref, send_ref)


def gram_of(left, right):
    tall = lax.dot_general(
        jnp.concatenate(thirds(left), axis=0), jnp.concatenate(thirds(right), axis=0),
        (((1,), (1,)), ((), ())), preferred_element_type=F32,
    )
    rows, cols = left.shape[0], right.shape[0]
    part = [[tall[i * rows : (i + 1) * rows, k * cols : (k + 1) * cols] for k in range(3)] for i in range(3)]
    small = (part[0][2] + part[2][0]) + part[1][1]
    return ((part[2][2] + (part[1][2] + part[2][1])) + small) + (part[0][1] + part[1][0]) + part[0][0]


def widen(gram, lanes):
    return jnp.concatenate([gram, jnp.zeros((gram.shape[0], lanes - gram.shape[1]), F32)], axis=1)


def project_both_body(days_all, pieces, chunks, par_ref, core_ref, *rest):
    halves_refs = rest[: 2 * pieces]
    block_refs = rest[2 * pieces : 2 * pieces + chunks]
    *out_refs, full_ref, out_ref = rest[2 * pieces + chunks :]
    start = 0
    for k in range(pieces):
        mine_ref, theirs_ref = halves_refs[2 * k : 2 * k + 2]
        lane_joined(par_ref, mine_ref, theirs_ref, full_ref, start)
        start += 2 * mine_ref.shape[1]
    applied = full_ref[...] / days_all
    days = block_refs[0].shape[0]
    projected = forward_project(applied, block_refs)
    gram = gram_of(applied, applied)
    half = out_ref.shape[0]
    for k in range(2):
        out_ref[:, :days] = projected[k * half : (k + 1) * half]
        out_ref[:, days:] = widen(gram[k * half : (k + 1) * half], LANES)
        halves(core_ref, out_ref, *out_refs[2 * k : 2 * k + 2])


def project_lead_body(days_all, par_ref, core_ref, mine_ref, theirs_ref, *rest):
    *block_refs, inv_ref, keep_ref, send_ref, raw_ref, applied_ref, full_ref, out_ref = rest
    lane_joined(par_ref, mine_ref, theirs_ref, full_ref)
    raw = full_ref[...] / days_all
    half = full_ref.shape[0]
    applied = jnp.dot(inv_ref[:half, :half], raw, precision=HIGH, preferred_element_type=F32)
    raw_ref[...] = raw
    applied_ref[...] = applied
    days = block_refs[0].shape[0]
    out_ref[:, :days] = forward_project(applied, block_refs)
    out_ref[:, days:] = widen(gram_of(applied, applied), LANES)
    halves(core_ref, out_ref, keep_ref, send_ref)


def project_trail_body(days_all, par_ref, core_ref, mine_ref, theirs_ref, raw_ref, lead_ref, *rest):
    *block_refs, inv_ref, keep_ref, send_ref, full_ref, out_ref = rest
    lane_joined(par_ref, mine_ref, theirs_ref, full_ref)
    half = full_ref.shape[0]
    raw = jnp.concatenate([raw_ref[...], full_ref[...] / days_all], axis=0)
    applied = jnp.dot(inv_ref[half:, :], raw, precision=HIGH, preferred_element_type=F32)
    days = block_refs[0].shape[0]
    out_ref[:, :days] = forward_project(applied, block_refs)
    both = jnp.concatenate([lead_ref[...], applied], axis=0)
    out_ref[:, days:] = widen(gram_of(applied, both), LANES)
    halves(core_ref, out_ref, keep_ref, send_ref)


def eliminate(gram):
    size = gram.shape[0]
    rows = lax.broadcasted_iota(jnp.int32, (size, 2 * size), 0)
    lanes = lax.broadcasted_iota(jnp.int32, (size, 2 * size), 1)
    work = jnp.concatenate([gram, jnp.zeros_like(gram)], axis=1)
    work = jnp.where(lanes == rows + size, 1.0, work)
    for first in range(0, size, GROUP):
        columns = [jnp.broadcast_to(work[:, first + j : first + j + 1], work.shape) for j in range(GROUP)]
        for j in range(GROUP):
            k = first + j
            inverse = 1.0 / columns[j][k : k + 1, :]
            below = jnp.where(rows > k, columns[j], 0.0)
            for later in range(j + 1, GROUP):
                columns[later] = columns[later] - below * (columns[later][k : k + 1, :] * inverse)
            work = work - below * (work[k : k + 1, :] * inverse)
    on_diag = jnp.where(lanes == rows, work, 0.0)
    pivots = jnp.sqrt(jnp.sum(on_diag, axis=1, keepdims=True))
    diag_row = jnp.sqrt(jnp.sum(on_diag, axis=0, keepdims=True))[:, :size]
    return work[:, size:] / pivots, diag_row


def factor_body(days, core_ref, mine_ref, theirs_ref, mine_late_ref, theirs_late_ref, inv_ref, diag_ref, full_ref):
    joined(core_ref, mine_ref, theirs_ref, full_ref)
    size = inv_ref.shape[0]
    half = size // 2
    lead = full_ref[:, days : days + half]
    joined(core_ref, mine_late_ref, theirs_late_ref, full_ref)
    trail = full_ref[:, days : days + size]
    top = jnp.concatenate([lead, trail[:, :half].T], axis=1)
    inverse, diag_row = eliminate(jnp.concatenate([top, trail], axis=0))
    inv_ref[...] = inverse
    diag_ref[...] = diag_row


def last_gram_body(days_all, lead_ref, trail_ref, inv_ref, applied_ref, gram_ref):
    raw = jnp.concatenate([lead_ref[...], trail_ref[...]], axis=0) / days_all
    applied = jnp.dot(inv_ref[...], raw, precision=HIGH, preferred_element_type=F32)
    applied_ref[...] = applied
    gram = gram_of(applied, applied)
    half = gram_ref.shape[0]
    gram_ref[...] = jnp.concatenate([gram[:half], gram[half:]], axis=1)


def last_body(scale, par_ref, mine_ref, theirs_ref, gram_ref, *rest):
    diag_refs = rest[: ITERS - 1]
    out_ref, strengths_ref, full_ref = rest[ITERS - 1 :]
    lane_joined(par_ref, mine_ref, theirs_ref, full_ref)
    factors = full_ref.shape[0]
    gram = jnp.concatenate([gram_ref[:, :factors], gram_ref[:, factors:]], axis=0)
    inverse, diag_row = eliminate(gram)
    out_ref[...] = jnp.dot(inverse, full_ref[...], precision=HIGH, preferred_element_type=F32) * scale
    for k, ref in enumerate(diag_refs):
        strengths_ref[k : k + 1, :] = ref[...]
    strengths_ref[ITERS - 1 : ITERS, :] = diag_row


def swap(x, axis, mask):
    size = lax.axis_size(axis)
    return lax.ppermute(x, axis, [(s, s ^ mask) for s in range(size)])


def cross(x, gr_mask, gc_mask):
    gr, gc = lax.axis_size("gr"), lax.axis_size("gc")
    pairs = [(g * gc + c, (g ^ gr_mask) * gc + (c ^ gc_mask)) for g in range(gr) for c in range(gc)]
    return lax.ppermute(x, ("gr", "gc"), pairs)


def tree(parts):
    while len(parts) > 1:
        parts = [parts[i] + parts[i + 1] for i in range(0, len(parts), 2)]
    return parts[0]


def sum_chips(x):
    size = lax.axis_size("gr")
    return tree([x if m == 0 else swap(x, "gr", m) for m in range(0, size, 2)])


def sum_days(keep, send):
    size = lax.axis_size("gc")
    mine = keep + swap(send, "gc", 1)
    mask = 2
    while mask < size:
        mine = mine + swap(mine, "gc", mask)
        mask *= 2
    return mine


def sum_assets(keep, send, reverse):
    mine = keep + swap(send, "gr", 1)
    size = lax.axis_size("gr")
    masks = [m for m in (1 << k for k in range(1, size)) if m < size]
    for mask in masks[::-1] if reverse else masks:
        mine = mine + swap(mine, "gr", mask)
    return mine, swap(mine, "gr", 1)


def local(returns, start_seed):
    days, assets = returns.shape
    factors = start_seed.shape[1]
    blocks, slabs = lax.axis_size("gr"), lax.axis_size("gc")
    span = assets // blocks
    slab_days = days * blocks
    days_all = slab_days * slabs
    core = (lax.axis_index("gr") % 2).astype(jnp.int32).reshape(1)
    par = (lax.axis_index("gc") % 2).astype(jnp.int32).reshape(1)
    me = lax.axis_index("gr").astype(jnp.int32).reshape(1)
    half = factors // 2
    packed_width = slab_days + LANES
    dots = 6 * factors * slab_days * span

    unit = 2 * LANES
    cut = span * CUT // 8 // unit * unit
    rest = span - cut

    own, *pieces, dealt = opening(me, returns, start_seed.T, blocks, cut)
    even = tuple(range(0, blocks, 2))
    near = [own if m == 0 else swap(own, "gr", m) for m in even]
    far = [swap(x, "gr", 1) for x in near]
    shared = [x for pair in zip(near, far) for x in pair]
    pieces = [p if m == 0 else swap(p, "gr", m) for m, p in enumerate(pieces)]
    last = lax.all_to_all(dealt, "gr", 0, 0).reshape(slab_days, rest)

    asset_half = ((factors, span // 2), F32)
    full_assets = pltpu.VMEM((factors, span), F32)
    slab = pltpu.VMEM((factors, slab_days), F32)

    block, keep, send = call(
        functools.partial(apply_first_body, blocks, True),
        [((slab_days, cut), BF16)] + [((factors, cut // 2), F32)] * 2, [me, par],
        shared + pieces, dots, [slab, pltpu.VMEM((factors, cut), F32)],
    )
    mine = sum_days(keep, send)
    theirs = swap(mine, "gc", 1)
    keep, send = call(
        functools.partial(apply_first_body, blocks, False), [((factors, rest // 2), F32)] * 2, [me, par],
        shared + [last], dots, [slab, pltpu.VMEM((factors, rest), F32)],
    )
    mine_late = sum_days(keep, send)
    pieces = [mine, theirs, mine_late, swap(mine_late, "gc", 1)]
    block_list = [block, last]
    quarter = ((half // 2, packed_width), F32)
    rows = ((half, span), F32)
    part_assets = pltpu.VMEM((half, span), F32)
    part_days = pltpu.VMEM((half, packed_width), F32)
    lane_half = ((half, span // 2), F32)
    diagonals = []
    for sweep in range(ITERS - 1):
        if sweep:
            mine = sum_days(*sent[0])
            keep, send, raw, applied = call(
                functools.partial(project_lead_body, days_all), [quarter] * 2 + [rows] * 2, [par, core],
                [mine, swap(mine, "gc", 1), *block_list, inverse], dots // 2, [part_assets, part_days],
            )
            lead = sum_assets(keep, send, False)
            mine = sum_days(*sent[1])
            keep, send = call(
                functools.partial(project_trail_body, days_all), [quarter] * 2, [par, core],
                [mine, swap(mine, "gc", 1), raw, applied, *block_list, inverse], dots // 2,
                [part_assets, part_days],
            )
            trail = sum_assets(keep, send, True)
        else:
            parts = call(
                functools.partial(project_both_body, days_all, len(pieces) // 2, len(block_list)),
                [quarter] * 4, [par, core], pieces + block_list, dots, [full_assets, part_days],
            )
            lead = sum_assets(*parts[:2], False)
            trail = sum_assets(*parts[2:], True)
        sent = [
            call(apply_body, [lane_half] * 2, [core, par], [*pair, *block_list], dots // 2, [part_days, part_assets])
            for pair in (lead, trail)
        ]
        inverse, diag_row = call(
            functools.partial(factor_body, slab_days),
            [((factors, factors), F32), ((1, factors), F32)], [core], [*lead, *trail], dots // 2, [part_days],
        )
        diagonals.append(diag_row)
    lead = sum_days(*sent[0])
    trail = sum_days(*sent[1])
    applied, gram = call(
        functools.partial(last_gram_body, days_all),
        [asset_half, ((half, 2 * factors), F32)], [], [lead, trail, inverse], dots,
    )
    theirs = swap(applied, "gc", 1)
    gram = (gram + cross(gram, 1, 0)) + (cross(gram, 0, 1) + cross(gram, 1, 1))
    gram = sum_chips(gram)
    loadings, strengths = call(
        functools.partial(last_body, math.sqrt(assets)),
        [((factors, span), F32), ((ITERS, factors), F32)], [par],
        [applied, theirs, gram, *diagonals], dots, [full_assets],
    )
    return loadings.T, strengths


def solution(mesh):
    placed = (P(("gr", "gc"), None), P())
    return jax.shard_map(local, mesh=mesh, in_specs=placed, out_specs=(P("gr", None), P()), check_vma=False)
```

```python
import functools
import math

import jax
import jax.numpy as jnp
from jax import lax
from jax.experimental import pallas as pl
from jax.experimental.pallas import tpu as pltpu
from jax.sharding import PartitionSpec as P

ITERS = 3
LANES = 128
GROUP = 16
CUT = 4
HIGH = lax.Precision.HIGHEST
F32 = jnp.float32
BF16 = jnp.bfloat16


def vmem(count):
    return [pl.BlockSpec(memory_space=pltpu.VMEM)] * count


def smem():
    return [pl.BlockSpec(memory_space=pltpu.SMEM)]


def call(body, outs, scalars, arrays, flops, scratch=()):
    in_specs = smem() * len(scalars) + vmem(len(arrays))
    moved = sum(math.prod(o[0]) * 4 for o in outs)
    return pl.pallas_call(
        body,
        out_shape=[jax.ShapeDtypeStruct(shape, dtype) for shape, dtype in outs],
        in_specs=in_specs,
        out_specs=vmem(len(outs)),
        scratch_shapes=list(scratch),
        cost_estimate=pl.CostEstimate(flops=flops, bytes_accessed=moved, transcendentals=0),
        compiler_params=pltpu.CompilerParams(vmem_limit_bytes=16 * 1024 * 1024),
    )(*scalars, *arrays)


def thirds(x):
    top = x.astype(BF16)
    rest = x - top.astype(F32)
    mid = rest.astype(BF16)
    low = (rest - mid.astype(F32)).astype(BF16)
    return top, mid, low


def fold(tall, rows):
    return tall[2 * rows :] + tall[rows : 2 * rows] + tall[:rows]


def open_body(me_ref, returns_ref, seed_ref, out_ref, *rest):
    *pieces, dealt_ref, wide_ref, table_ref, sems = rest
    blocks, _, width = dealt_ref.shape
    span = returns_ref.shape[1] // blocks
    copies = [
        pltpu.make_async_copy(returns_ref, wide_ref, sems.at[0]),
        pltpu.make_async_copy(seed_ref, table_ref, sems.at[1]),
    ]
    for mask, piece in enumerate(pieces):
        at = pl.multiple_of((me_ref[0] ^ mask) * span, LANES)
        source = returns_ref.at[:, pl.ds(at, piece.shape[1])]
        copies.append(pltpu.make_async_copy(source, piece, sems.at[2 + mask]))
    for copy in copies:
        copy.start()
    copies[0].wait()
    deals = [
        pltpu.make_async_copy(
            wide_ref.at[:, (b + 1) * span - width : (b + 1) * span], dealt_ref.at[b], sems.at[2 + blocks + b]
        )
        for b in range(blocks)
    ]
    for deal in deals:
        deal.start()
    copies[1].wait()
    factors = out_ref.shape[0]
    seed = table_ref[...]
    coarse = (seed >> 3) << 3
    fine = seed - coarse
    both = jnp.concatenate([coarse.astype(F32).astype(BF16), fine.astype(F32).astype(BF16)], axis=0)
    tall = lax.dot_general(both, wide_ref[...], (((1,), (1,)), ((), ())), preferred_element_type=F32)
    out_ref[...] = (tall[:factors] + tall[factors:]) / 1000.0
    for copy in copies[2:] + deals:
        copy.wait()


def opening(me, returns, seed, blocks, width):
    days, assets = returns.shape
    rest = assets // blocks - width
    factors = seed.shape[0]
    outs = [((factors, days), F32)] + [((days, width), BF16)] * blocks + [((blocks, days, rest), BF16)]
    return pl.pallas_call(
        open_body,
        out_shape=[jax.ShapeDtypeStruct(shape, dtype) for shape, dtype in outs],
        in_specs=smem() + [pl.BlockSpec(memory_space=pltpu.HBM)] * 2,
        out_specs=vmem(len(outs) - 1) + [pl.BlockSpec(memory_space=pltpu.HBM)],
        scratch_shapes=[
            pltpu.VMEM(returns.shape, BF16),
            pltpu.VMEM(seed.shape, jnp.int32),
            pltpu.SemaphoreType.DMA((2 + 2 * blocks,)),
        ],
        cost_estimate=pl.CostEstimate(
            flops=4 * days * assets * factors, bytes_accessed=returns.size * 2, transcendentals=0
        ),
        compiler_params=pltpu.CompilerParams(vmem_limit_bytes=51 * 1024 * 1024),
    )(me, returns, seed)


def halves(par_ref, full_ref, keep_ref, send_ref):
    rows = keep_ref.shape[0]
    at = pl.multiple_of(par_ref[0] * rows, 8)
    other = pl.multiple_of((1 - par_ref[0]) * rows, 8)
    keep_ref[...] = full_ref[pl.ds(at, rows), :]
    send_ref[...] = full_ref[pl.ds(other, rows), :]


def joined(par_ref, mine_ref, theirs_ref, full_ref):
    rows = mine_ref.shape[0]
    at = pl.multiple_of(par_ref[0] * rows, 8)
    other = pl.multiple_of((1 - par_ref[0]) * rows, 8)
    full_ref[pl.ds(at, rows), :] = mine_ref[...]
    full_ref[pl.ds(other, rows), :] = theirs_ref[...]


def lane_halves(par_ref, full_ref, keep_ref, send_ref):
    lanes = keep_ref.shape[1]
    at = pl.multiple_of(par_ref[0] * lanes, LANES)
    other = pl.multiple_of((1 - par_ref[0]) * lanes, LANES)
    keep_ref[...] = full_ref[:, pl.ds(at, lanes)]
    send_ref[...] = full_ref[:, pl.ds(other, lanes)]


def lane_joined(par_ref, mine_ref, theirs_ref, full_ref, start=0):
    lanes = mine_ref.shape[1]
    at = pl.multiple_of(start + par_ref[0] * lanes, LANES)
    other = pl.multiple_of(start + (1 - par_ref[0]) * lanes, LANES)
    full_ref[:, pl.ds(at, lanes)] = mine_ref[...]
    full_ref[:, pl.ds(other, lanes)] = theirs_ref[...]


def spans(block_refs):
    start, found = 0, []
    for ref in block_refs:
        found.append((start, ref))
        start += ref.shape[1]
    return found


def back_project(projected, block_refs, full_ref):
    parts = jnp.concatenate(thirds(projected), axis=0)
    for start, ref in spans(block_refs):
        tall = jnp.dot(parts, ref[...], preferred_element_type=F32)
        full_ref[:, start : start + ref.shape[1]] = fold(tall, projected.shape[0])


def forward_project(applied, block_refs):
    total = 0.0
    for start, ref in spans(block_refs):
        parts = jnp.concatenate(thirds(applied[:, start : start + ref.shape[1]]), axis=0)
        tall = lax.dot_general(parts, ref[...], (((1,), (1,)), ((), ())), preferred_element_type=F32)
        total = total + fold(tall, applied.shape[0])
    return total


def apply_first_body(count, gathered, me_ref, par_ref, *rest):
    slabs, rest = rest[:count], rest[count:]
    me = me_ref[0]
    days = slabs[0].shape[1]

    def source(mask):
        return pl.ds(pl.multiple_of((me ^ mask) * days, LANES), days)

    if gathered:
        *pieces, block_ref, keep_ref, send_ref, proj_ref, full_ref = rest
        for mask, piece in enumerate(pieces):
            block_ref[source(mask), :] = piece[...]
    else:
        block_ref, keep_ref, send_ref, proj_ref, full_ref = rest
    for mask, ref in enumerate(slabs):
        proj_ref[:, source(mask)] = ref[...]
    back_project(proj_ref[...], [block_ref], full_ref)
    lane_halves(par_ref, full_ref, keep_ref, send_ref)


def apply_body(core_ref, par_ref, mine_ref, theirs_ref, *rest):
    *block_refs, keep_ref, send_ref, proj_ref, full_ref = rest
    joined(core_ref, mine_ref, theirs_ref, proj_ref)
    back_project(proj_ref[:, : block_refs[0].shape[0]], block_refs, full_ref)
    lane_halves(par_ref, full_ref, keep_ref, send_ref)


def gram_of(left, right):
    tall = lax.dot_general(
        jnp.concatenate(thirds(left), axis=0), jnp.concatenate(thirds(right), axis=0),
        (((1,), (1,)), ((), ())), preferred_element_type=F32,
    )
    rows, cols = left.shape[0], right.shape[0]
    part = [[tall[i * rows : (i + 1) * rows, k * cols : (k + 1) * cols] for k in range(3)] for i in range(3)]
    small = (part[0][2] + part[2][0]) + part[1][1]
    return ((part[2][2] + (part[1][2] + part[2][1])) + small) + (part[0][1] + part[1][0]) + part[0][0]


def widen(gram, lanes):
    return jnp.concatenate([gram, jnp.zeros((gram.shape[0], lanes - gram.shape[1]), F32)], axis=1)


def project_both_body(days_all, pieces, chunks, par_ref, core_ref, *rest):
    halves_refs = rest[: 2 * pieces]
    block_refs = rest[2 * pieces : 2 * pieces + chunks]
    *out_refs, full_ref, out_ref = rest[2 * pieces + chunks :]
    start = 0
    for k in range(pieces):
        mine_ref, theirs_ref = halves_refs[2 * k : 2 * k + 2]
        lane_joined(par_ref, mine_ref, theirs_ref, full_ref, start)
        start += 2 * mine_ref.shape[1]
    applied = full_ref[...] / days_all
    days = block_refs[0].shape[0]
    projected = forward_project(applied, block_refs)
    gram = gram_of(applied, applied)
    half = out_ref.shape[0]
    for k in range(2):
        out_ref[:, :days] = projected[k * half : (k + 1) * half]
        out_ref[:, days:] = widen(gram[k * half : (k + 1) * half], LANES)
        halves(core_ref, out_ref, *out_refs[2 * k : 2 * k + 2])


def project_lead_body(days_all, par_ref, core_ref, mine_ref, theirs_ref, *rest):
    *block_refs, keep_ref, send_ref, applied_ref, full_ref, out_ref = rest
    lane_joined(par_ref, mine_ref, theirs_ref, full_ref)
    applied = full_ref[...] / days_all
    applied_ref[...] = applied
    days = block_refs[0].shape[0]
    out_ref[:, :days] = forward_project(applied, block_refs)
    out_ref[:, days:] = widen(gram_of(applied, applied), LANES)
    halves(core_ref, out_ref, keep_ref, send_ref)


def project_trail_body(days_all, par_ref, core_ref, mine_ref, theirs_ref, lead_ref, *rest):
    *block_refs, keep_ref, send_ref, full_ref, out_ref = rest
    lane_joined(par_ref, mine_ref, theirs_ref, full_ref)
    applied = full_ref[...] / days_all
    days = block_refs[0].shape[0]
    out_ref[:, :days] = forward_project(applied, block_refs)
    both = jnp.concatenate([lead_ref[...], applied], axis=0)
    out_ref[:, days:] = widen(gram_of(applied, both), LANES)
    halves(core_ref, out_ref, keep_ref, send_ref)


def apply_scaled_body(core_ref, par_ref, mine_ref, theirs_ref, mine_late_ref, theirs_late_ref, inv_ref, *rest):
    *block_refs, keep_ref, send_ref, keep_late_ref, send_late_ref, proj_ref, full_ref = rest
    half = keep_ref.shape[0]
    days = block_refs[0].shape[0]
    joined(core_ref, mine_ref, theirs_ref, proj_ref)
    lead = proj_ref[:, :days]
    joined(core_ref, mine_late_ref, theirs_late_ref, proj_ref)
    both = jnp.concatenate([lead, proj_ref[:, :days]], axis=0)
    scaled = jnp.dot(inv_ref[...], both, precision=HIGH, preferred_element_type=F32)
    back_project(scaled, block_refs, full_ref)
    lane_halves(par_ref, full_ref.at[:half], keep_ref, send_ref)
    lane_halves(par_ref, full_ref.at[half:], keep_late_ref, send_late_ref)


def eliminate(gram):
    size = gram.shape[0]
    rows = lax.broadcasted_iota(jnp.int32, (size, 2 * size), 0)
    lanes = lax.broadcasted_iota(jnp.int32, (size, 2 * size), 1)
    work = jnp.concatenate([gram, jnp.zeros_like(gram)], axis=1)
    work = jnp.where(lanes == rows + size, 1.0, work)
    for first in range(0, size, GROUP):
        columns = [jnp.broadcast_to(work[:, first + j : first + j + 1], work.shape) for j in range(GROUP)]
        for j in range(GROUP):
            k = first + j
            inverse = 1.0 / columns[j][k : k + 1, :]
            below = jnp.where(rows > k, columns[j], 0.0)
            for later in range(j + 1, GROUP):
                columns[later] = columns[later] - below * (columns[later][k : k + 1, :] * inverse)
            work = work - below * (work[k : k + 1, :] * inverse)
    on_diag = jnp.where(lanes == rows, work, 0.0)
    pivots = jnp.sqrt(jnp.sum(on_diag, axis=1, keepdims=True))
    diag_row = jnp.sqrt(jnp.sum(on_diag, axis=0, keepdims=True))[:, :size]
    return work[:, size:] / pivots, diag_row


def factor_body(days, core_ref, mine_ref, theirs_ref, mine_late_ref, theirs_late_ref, inv_ref, diag_ref, full_ref):
    joined(core_ref, mine_ref, theirs_ref, full_ref)
    size = inv_ref.shape[0]
    half = size // 2
    lead = full_ref[:, days : days + half]
    joined(core_ref, mine_late_ref, theirs_late_ref, full_ref)
    trail = full_ref[:, days : days + size]
    top = jnp.concatenate([lead, trail[:, :half].T], axis=1)
    inverse, diag_row = eliminate(jnp.concatenate([top, trail], axis=0))
    inv_ref[...] = inverse
    diag_ref[...] = diag_row


def last_gram_body(days_all, lead_ref, trail_ref, inv_ref, applied_ref, gram_ref):
    raw = jnp.concatenate([lead_ref[...], trail_ref[...]], axis=0) / days_all
    applied = jnp.dot(inv_ref[...], raw, precision=HIGH, preferred_element_type=F32)
    applied_ref[...] = applied
    gram = gram_of(applied, applied)
    half = gram_ref.shape[0]
    gram_ref[...] = jnp.concatenate([gram[:half], gram[half:]], axis=1)


def last_body(scale, par_ref, mine_ref, theirs_ref, gram_ref, *rest):
    diag_refs = rest[: ITERS - 1]
    out_ref, strengths_ref, full_ref = rest[ITERS - 1 :]
    lane_joined(par_ref, mine_ref, theirs_ref, full_ref)
    factors = full_ref.shape[0]
    gram = jnp.concatenate([gram_ref[:, :factors], gram_ref[:, factors:]], axis=0)
    inverse, diag_row = eliminate(gram)
    out_ref[...] = jnp.dot(inverse, full_ref[...], precision=HIGH, preferred_element_type=F32) * scale
    for k, ref in enumerate(diag_refs):
        strengths_ref[k : k + 1, :] = ref[...]
    strengths_ref[ITERS - 1 : ITERS, :] = diag_row


def swap(x, axis, mask):
    size = lax.axis_size(axis)
    return lax.ppermute(x, axis, [(s, s ^ mask) for s in range(size)])


def cross(x, gr_mask, gc_mask):
    gr, gc = lax.axis_size("gr"), lax.axis_size("gc")
    pairs = [(g * gc + c, (g ^ gr_mask) * gc + (c ^ gc_mask)) for g in range(gr) for c in range(gc)]
    return lax.ppermute(x, ("gr", "gc"), pairs)


def tree(parts):
    while len(parts) > 1:
        parts = [parts[i] + parts[i + 1] for i in range(0, len(parts), 2)]
    return parts[0]


def sum_chips(x):
    size = lax.axis_size("gr")
    return tree([x if m == 0 else swap(x, "gr", m) for m in range(0, size, 2)])


def sum_days(keep, send):
    size = lax.axis_size("gc")
    mine = keep + swap(send, "gc", 1)
    mask = 2
    while mask < size:
        mine = mine + swap(mine, "gc", mask)
        mask *= 2
    return mine


def sum_assets(keep, send, reverse):
    mine = keep + swap(send, "gr", 1)
    size = lax.axis_size("gr")
    masks = [m for m in (1 << k for k in range(1, size)) if m < size]
    for mask in masks[::-1] if reverse else masks:
        mine = mine + swap(mine, "gr", mask)
    return mine, swap(mine, "gr", 1)


def local(returns, start_seed):
    days, assets = returns.shape
    factors = start_seed.shape[1]
    blocks, slabs = lax.axis_size("gr"), lax.axis_size("gc")
    span = assets // blocks
    slab_days = days * blocks
    days_all = slab_days * slabs
    core = (lax.axis_index("gr") % 2).astype(jnp.int32).reshape(1)
    par = (lax.axis_index("gc") % 2).astype(jnp.int32).reshape(1)
    me = lax.axis_index("gr").astype(jnp.int32).reshape(1)
    half = factors // 2
    packed_width = slab_days + LANES
    dots = 6 * factors * slab_days * span

    unit = 2 * LANES
    cut = span * CUT // 8 // unit * unit
    rest = span - cut

    own, *pieces, dealt = opening(me, returns, start_seed.T, blocks, cut)
    even = tuple(range(0, blocks, 2))
    near = [own if m == 0 else swap(own, "gr", m) for m in even]
    far = [swap(x, "gr", 1) for x in near]
    shared = [x for pair in zip(near, far) for x in pair]
    pieces = [p if m == 0 else swap(p, "gr", m) for m, p in enumerate(pieces)]
    last = lax.all_to_all(dealt, "gr", 0, 0).reshape(slab_days, rest)

    asset_half = ((factors, span // 2), F32)
    full_assets = pltpu.VMEM((factors, span), F32)
    slab = pltpu.VMEM((factors, slab_days), F32)

    block, keep, send = call(
        functools.partial(apply_first_body, blocks, True),
        [((slab_days, cut), BF16)] + [((factors, cut // 2), F32)] * 2, [me, par],
        shared + pieces, dots, [slab, pltpu.VMEM((factors, cut), F32)],
    )
    mine = sum_days(keep, send)
    theirs = swap(mine, "gc", 1)
    keep, send = call(
        functools.partial(apply_first_body, blocks, False), [((factors, rest // 2), F32)] * 2, [me, par],
        shared + [last], dots, [slab, pltpu.VMEM((factors, rest), F32)],
    )
    mine_late = sum_days(keep, send)
    pieces = [mine, theirs, mine_late, swap(mine_late, "gc", 1)]
    block_list = [block, last]
    quarter = ((half // 2, packed_width), F32)
    rows = ((half, span), F32)
    part_assets = pltpu.VMEM((half, span), F32)
    part_days = pltpu.VMEM((half, packed_width), F32)
    lane_half = ((half, span // 2), F32)
    diagonals = []
    for sweep in range(ITERS - 1):
        if sweep:
            mine = sum_days(*sent[0])
            keep, send, applied = call(
                functools.partial(project_lead_body, days_all), [quarter] * 2 + [rows], [par, core],
                [mine, swap(mine, "gc", 1), *block_list], dots // 2, [part_assets, part_days],
            )
            lead = sum_assets(keep, send, False)
            mine = sum_days(*sent[1])
            keep, send = call(
                functools.partial(project_trail_body, days_all), [quarter] * 2, [par, core],
                [mine, swap(mine, "gc", 1), applied, *block_list], dots // 2,
                [part_assets, part_days],
            )
            trail = sum_assets(keep, send, True)
        else:
            parts = call(
                functools.partial(project_both_body, days_all, len(pieces) // 2, len(block_list)),
                [quarter] * 4, [par, core], pieces + block_list, dots, [full_assets, part_days],
            )
            lead = sum_assets(*parts[:2], False)
            trail = sum_assets(*parts[2:], True)
        inverse, diag_row = call(
            functools.partial(factor_body, slab_days),
            [((factors, factors), F32), ((1, factors), F32)], [core], [*lead, *trail], dots // 2, [part_days],
        )
        if sweep == 0:
            outs = call(
                apply_scaled_body, [lane_half] * 4, [core, par], [*lead, *trail, inverse, *block_list], dots,
                [part_days, full_assets],
            )
            sent = [outs[:2], outs[2:]]
        else:
            sent = [
                call(apply_body, [lane_half] * 2, [core, par], [*pair, *block_list], dots // 2, [part_days, part_assets])
                for pair in (lead, trail)
            ]
        diagonals.append(diag_row)
    lead = sum_days(*sent[0])
    trail = sum_days(*sent[1])
    applied, gram = call(
        functools.partial(last_gram_body, days_all),
        [asset_half, ((half, 2 * factors), F32)], [], [lead, trail, inverse], dots,
    )
    theirs = swap(applied, "gc", 1)
    gram = (gram + cross(gram, 1, 0)) + (cross(gram, 0, 1) + cross(gram, 1, 1))
    gram = sum_chips(gram)
    loadings, strengths = call(
        functools.partial(last_body, math.sqrt(assets)),
        [((factors, span), F32), ((ITERS, factors), F32)], [par],
        [applied, theirs, gram, *diagonals], dots, [full_assets],
    )
    return loadings.T, strengths


def solution(mesh):
    placed = (P(("gr", "gc"), None), P())
    return jax.shard_map(local, mesh=mesh, in_specs=placed, out_specs=(P("gr", None), P()), check_vma=False)
```
